256 devices in a mesh: gx: 8 (over x, core), gy: 8 (over z), gz: 4 (over y).
Axes of the slice: x: 4, y: 4, z: 8, core: 2. Of those that a mesh axis runs over, the one named last changes fastest.
Arguments:
- pair_list: int32 [8192, 2], P(('gx', 'gy', 'gz')), may hold values from 0 to 63, all different within a row; in each aligned block of 32 rows (0 to 31, 32 to 63, ...) at most 2 rows name the same one
- rank_bucket: int32 [8192], P(('gx', 'gy', 'gz')), may hold values from 0 to 2
- amplitudes: bfloat16 [8192, 36864], P(('gx', 'gy', 'gz')), may hold values from -0.4375 to 0.4375
- intersects: bfloat16 [8192, 36864], P(('gx', 'gy', 'gz')), may hold values from -0.4375 to 0.4375
- integrals: bfloat16 [8192, 36864], P(('gx', 'gy', 'gz')), may hold values from -6 to 6
- exchange_blocks: bfloat16 [64, 36864], P(('gx', 'gy')), may hold values from -0.4375 to 0.4375
Outputs:
- residuals: bfloat16 [8192, 36864], P(('gx', 'gy', 'gz'))
The draws below stay inside these ranges and needn't reach their ends.
Inputs may be any that keep to these rules, and one draw needn't show every extreme that they name: `pair_list`: each row names two different occupied orbitals; within the rows of one device no orbital is named more than 2 times, a bound that some block reaches on some devices. `rank_bucket`: bucket b keeps the leading (b + 1) * 64 PNOs.
All inputs are finite; a program needn't handle non-finite values.
Results may differ from the reference program's by a relative error of at most 0.013.
Values may be sent and summed in bfloat16 or wider, within the bound.
No kernel may reach another device: no remote copies, remote signals or barrier semaphores. Data moves between devices by JAX's collectives and lax.ppermute only.
A program may use at most 128 MiB of HBM per device.

```python
import math
import jax
import jax.numpy as jnp
import numpy as np
from jax import lax

RSTEP = 64
R = 192
NOCC = 64
MOST = 2
PAIR_DEV = 32
NPAIRS = 8192


def touch_ends(values, stream_key, least, top_value):
    place = [jax.random.randint(jax.random.fold_in(stream_key, axis), (), 0, length) for axis, length in enumerate(values.shape)]
    main_axis = values.shape.index(max(values.shape))
    neighbour = place[:main_axis] + [(place[main_axis] + 1) % values.shape[main_axis]] + place[main_axis + 1:]
    return values.at[tuple(place)].set(least).at[tuple(neighbour)].set(top_value)


def levels(key, shape, split, least, high):
    def one(dim, parts):
        heights = jax.random.uniform(jax.random.fold_in(jax.random.fold_in(key, 6), dim), (parts,), jnp.float32, least / len(split), high / len(split))
        return jnp.repeat(jnp.exp(heights), shape[dim] // parts).reshape((-1,) + (1,) * (len(shape) - dim - 1))

    gain = one(*split[0])
    for cut in split[1:]:
        gain = gain * one(*cut)
    return gain


def deal_out(rng, own, number, rows, amount, top, bound, lean):
    order = jax.random.permutation(rng, amount)
    heavy_load, ordinary = load_shares(amount, rows * top, bound, lean, True), load_shares(amount, rows * top, bound, lean, False)
    places = jnp.arange(amount)

    def named(tallies, turn):
        used = int((tallies > 0).sum())
        fixed = max(1, used // 4)
        passed = fixed + (places - fixed + turn * (used - fixed)) % max(1, amount - fixed)
        return jnp.zeros((amount,), jnp.int32).at[order[jnp.where(places < fixed, places, passed)]].set(jnp.asarray(tallies, jnp.int32))

    tallies = jnp.where(number % 4 == 0, named(heavy_load, number // 4), named(ordinary, number - number // 4 - 1))
    mixed = jax.random.permutation(jax.random.fold_in(own, 3), amount)
    giver, receiver = mixed[0:amount // 2 * 2:2], mixed[1:amount // 2 * 2:2]
    slack = jnp.minimum(tallies[giver] - 1, bound - tallies[receiver]) // 2
    slack = jnp.where((giver == order[0]) | (receiver == order[0]) | (tallies[receiver] == 0), 0, jnp.maximum(slack, 0))
    passed = jax.random.randint(jax.random.fold_in(own, 4), (amount // 2,), 0, 1 << 20) % (slack + 1)
    tallies = tallies.at[giver].add(-passed).at[receiver].add(passed)
    items = jnp.searchsorted(jnp.cumsum(tallies), jnp.arange(rows * top), side="right").astype(jnp.int32)
    listing = items.reshape(top, rows).T
    listing = listing[jax.random.permutation(jax.random.fold_in(own, 1), rows)]
    turn = jax.random.randint(jax.random.fold_in(own, 2), (rows, 1), 0, top)
    return jnp.take_along_axis(listing, (jnp.arange(top)[None, :] + turn) % top, axis=1)


def load_shares(count, total, bound, slope, full):
    portions = [(1 << 20) // math.isqrt(standing ** slope) + 1 for standing in range(1, count + 1)]
    largest = bound if full else min(bound, max(-(-total // count), total * portions[0] // sum(portions)))
    least = 1 if total - largest >= count - 1 else 0
    holding, surplus = [largest] + [least] * (count - 1), total - largest - least * (count - 1)
    while surplus > 0:
        movable = [i for i in range(1, count) if holding[i] < largest] or [i for i in range(1, count) if holding[i] < bound]
        pool, remaining = sum([portions[i] for i in movable]), surplus
        for i in movable:
            extra = min(bound - holding[i], max(1, remaining * portions[i] // pool), surplus)
            holding[i] = holding[i] + extra
            surplus = surplus - extra
    return np.array(holding)


def scatter_about(rng, shape, scale, limit, cuts=(), kind=jnp.bfloat16):
    values = scale * jax.random.normal(rng, shape, jnp.float32)
    if cuts:
        values = values * levels(rng, shape, cuts, -0.22, 0.18)
    return jnp.clip(values, -limit, limit).astype(kind)


def setup_inputs(seed: int = 0) -> dict:
    keys = jax.random.split(jax.random.key(seed), 7)
    pair_list_keys = jax.random.split(jax.random.fold_in(keys[0], 1), NPAIRS // PAIR_DEV)
    pair_list_turns = jax.random.permutation(jax.random.fold_in(keys[0], 3), NPAIRS // PAIR_DEV)
    pair_list = jax.vmap(lambda own, number: deal_out(jax.random.fold_in(keys[0], 2), own, number, PAIR_DEV, NOCC, 2, MOST, 2))(pair_list_keys, pair_list_turns).reshape((NPAIRS, 2))
    rank_bucket = touch_ends(jax.random.randint(keys[1], (NPAIRS,), 0, 3), jax.random.fold_in(keys[1], 1), 0, 2).astype(jnp.int32)
    amplitudes = scatter_about(keys[2], (NPAIRS, R * R), R ** -0.5, 0.4375, ((0, 256),))
    intersects = scatter_about(keys[3], (NPAIRS, R * R), R ** -0.5, 0.4375, ((0, 256),))
    integrals = scatter_about(keys[4], (NPAIRS, R * R), 1.0, 6.0, ((0, 256),))
    exchange_blocks = scatter_about(keys[5], (NOCC, R * R), R ** -0.5, 0.4375, ((0, 64),))
    return {"pair_list": pair_list, "rank_bucket": rank_bucket, "amplitudes": amplitudes, "intersects": intersects, "integrals": integrals, "exchange_blocks": exchange_blocks}


def rounded(value):
    return lax.optimization_barrier(value.astype(jnp.bfloat16)).astype(jnp.float32)


def rank_mask(bucket):
    rank_size = (bucket + 1) * RSTEP
    row_index = jnp.arange(R, dtype=jnp.int32)
    return (row_index[None, :, None] < rank_size[:, None, None]) & (row_index[None, None, :] < rank_size[:, None, None])


def project_block(inputs):
    bucket, amplitude, intersect = inputs
    inside = rank_mask(bucket)
    masked = jnp.where(inside, amplitude, jnp.zeros_like(amplitude))
    half_projected = rounded(jnp.einsum('pab,pbc->pac', intersect.astype(jnp.float32), masked.astype(jnp.float32)))
    return jnp.einsum('pab,pcb->pac', half_projected, intersect.astype(jnp.float32)).astype(jnp.bfloat16)


def reference(pair_list, rank_bucket, amplitudes, intersects, integrals, exchange_blocks):
    blocks = NPAIRS // PAIR_DEV
    block_shape = (blocks, PAIR_DEV, R, R)
    exchange_square = exchange_blocks.reshape(NOCC, R, R)
    bucket_blocks = rank_bucket.reshape(blocks, PAIR_DEV)
    list_blocks = pair_list.reshape(blocks, PAIR_DEV, 2)
    amplitude_blocks = amplitudes.reshape(block_shape)
    intersect_blocks = intersects.reshape(block_shape)
    integral_blocks = integrals.reshape(block_shape)
    projected = lax.map(project_block, (bucket_blocks, amplitude_blocks, intersect_blocks))

    def accumulate(domain, inputs):
        ends_block, projected_block = inputs
        as_float = projected_block.astype(jnp.float32)
        domain = domain + jax.ops.segment_sum(as_float, ends_block[:, 0], num_segments=NOCC)
        domain = domain + jax.ops.segment_sum(as_float, ends_block[:, 1], num_segments=NOCC)
        return domain, None

    domain, unused = lax.scan(accumulate, jnp.zeros((NOCC, R, R), jnp.float32), (list_blocks, projected))
    coupled = rounded(jnp.einsum('oab,obc->oac', rounded(domain), exchange_square.astype(jnp.float32)))

    def finish(inputs):
        ends_block, bucket, projected_block, intersect, integral, amplitude = inputs
        inside = rank_mask(bucket)
        masked = jnp.where(inside, amplitude, jnp.zeros_like(amplitude))
        combined = jnp.zeros((PAIR_DEV, R, R), jnp.float32)
        for which_end in range(2):
            orbital = ends_block[:, which_end]
            own_term = rounded(jnp.einsum('pab,pbc->pac', projected_block.astype(jnp.float32), exchange_square[orbital].astype(jnp.float32)))
            answer = rounded(coupled[orbital] - own_term)
            combined = combined + answer
        combined = rounded(combined)
        half_back = rounded(jnp.einsum('pba,pbc->pac', intersect.astype(jnp.float32), combined))
        back_projected = jnp.einsum('pab,pbc->pac', half_back, intersect.astype(jnp.float32))
        local_term = jnp.einsum('pab,pbc->pac', masked.astype(jnp.float32), integral.astype(jnp.float32))
        residual_sum = integral.astype(jnp.float32) + local_term + back_projected
        return jnp.where(inside, residual_sum, jnp.zeros_like(residual_sum)).astype(jnp.bfloat16)

    result = lax.map(finish, (list_blocks, bucket_blocks, projected, intersect_blocks, integral_blocks, amplitude_blocks))
    return result.reshape(NPAIRS, R * R)
```

```python
import functools
import jax
import jax.numpy as jnp
from jax import lax
from jax.experimental import pallas as pl
from jax.experimental.pallas import tpu as pltpu
from jax.sharding import Mesh
from jax.sharding import PartitionSpec as P

RSTEP = 64
R = 192
Q = 48
QP = 72
STEP = 4
AXES = ("gx_0", "gx_1", "gy", "gz")
GX_GY = ("gx_0", "gx_1", "gy")
BF16 = jnp.bfloat16
F32 = jnp.float32


def device_number(x, c, z, y):
    return ((x * 2 + c) * 8 + z) * 4 + y


def pairs_of(move):
    out = []
    for x in range(4):
        for c in range(2):
            for z in range(8):
                for y in range(4):
                    out.append((device_number(x, c, z, y), device_number(*move(x, c, z, y))))
    return out


def stage_a(array, d):
    return lax.ppermute(
        array, AXES, pairs_of(lambda x, c, z, y: (x ^ d, c, z, y) if c == 0 else (x, c, z, y ^ d))
    )


def stage_b(array, d):
    return lax.ppermute(
        array, AXES, pairs_of(lambda x, c, z, y: (x, c, z, y ^ d) if c == 0 else (x ^ d, c, z, y))
    )


def stage_z(array, d):
    return lax.ppermute(array, AXES, pairs_of(lambda x, c, z, y: (x, c, z ^ d, y)))


def stage_c(array):
    return lax.ppermute(array, AXES, pairs_of(lambda x, c, z, y: (x, c ^ 1, z, y)))


def slot_of(k, q, at_ref):
    x, c, z, y = (at_ref[i] for i in range(4))
    core = (k >> 3) & 1
    dx, dq, dz = (k >> 4) ^ x, q ^ y, (k & 7) ^ z
    a = jnp.where(core == 0, dx, dq)
    b = jnp.where(core == 0, dq, dx)
    return (((core ^ c) * 4 + a) * 4 + b) * 8 + (dz & 1) * 4 + (dz >> 1)


def packed_quarter(block, q):
    rows = block[q * Q : (q + 1) * Q]
    right = jnp.concatenate([rows[: Q // 2, 128:], rows[Q // 2 :, 128:]], axis=1)
    return jnp.concatenate([rows[:, :128], right], axis=0)


def unpacked_quarter(piece):
    right = piece[Q:]
    right = jnp.concatenate([right[:, :64], right[:, 64:]], axis=0)
    return jnp.concatenate([piece[:Q], right], axis=1)


def masks(rank):
    rows = lax.broadcasted_iota(jnp.int32, (R, R), 0)
    cols = lax.broadcasted_iota(jnp.int32, (R, R), 1)
    return (rows < rank) & (cols < rank)


def dot(a, b, dims):
    return lax.dot_general(a, b, (dims, ((), ())), preferred_element_type=F32)


def project_kernel(ends_ref, rank_ref, at_ref, s_ref, m_ref, p_ref, *rest):
    out_refs, sums_ref = rest[:8], rest[8]
    step = pl.program_id(0)

    @pl.when(step == 0)
    def _():
        sums_ref[...] = jnp.zeros_like(sums_ref)

    for i in range(STEP):
        pair = step * STEP + i
        inside = masks((rank_ref[pair] + 1) * RSTEP)
        masked = jnp.where(inside, m_ref[i].astype(F32), 0.0).astype(BF16)
        half = dot(s_ref[i], masked, ((1,), (0,))).astype(BF16)
        full = dot(half, s_ref[i], ((1,), (1,)))
        p_ref[i] = full.astype(BF16)
        for q in range(4):
            piece = packed_quarter(full, q).astype(BF16)
            for e in range(2):
                slot = slot_of(ends_ref[pair * 2 + e], q, at_ref)
                sums_ref[slot] = sums_ref[slot] + piece

    @pl.when(step == pl.num_programs(0) - 1)
    def _():
        for n in range(8):
            out_refs[n][...] = sums_ref[n * 32 : (n + 1) * 32].reshape(4, 8, QP, 128)


def whole(shape):
    return pl.BlockSpec(shape, lambda *_: (0,) * len(shape))


def project(ends, rank, at, s, m):
    pairs = s.shape[0]
    block = pl.BlockSpec((STEP, R, R), lambda i, *_: (i, 0, 0))
    group = (4, 8, QP, 128)
    return pl.pallas_call(
        project_kernel,
        grid_spec=pltpu.PrefetchScalarGridSpec(
            num_scalar_prefetch=3,
            grid=(pairs // STEP,),
            in_specs=[block, block],
            out_specs=[block] + [whole(group)] * 8,
            scratch_shapes=[pltpu.VMEM((256, QP, 128), BF16)],
        ),
        out_shape=[jax.ShapeDtypeStruct((pairs, R, R), BF16)]
        + [jax.ShapeDtypeStruct(group, BF16)] * 8,
        cost_estimate=pl.CostEstimate(
            flops=pairs * 4 * R**3, transcendentals=0, bytes_accessed=pairs * 6 * R * R
        ),
        name="project",
    )(ends, rank, at, s, m)


def unpack_kernel(at_ref, *refs):
    out_ref = refs[8]
    x, c, z, y = (at_ref[i] for i in range(4))
    for n in range(8):
        core, a = (n // 4) ^ c, n % 4

        def piece(i, _, n=n, core=core, a=a):
            b, j = i // 8, i % 8
            dx = jnp.where(core == 0, a, b)
            dq = jnp.where(core == 0, b, a)
            k = ((dx ^ x) * 2 + core) * 8 + ((((j & 3) << 1) | (j >> 2)) ^ z)
            rows = pl.multiple_of((dq ^ y) * Q, Q)
            out_ref[k, pl.ds(rows, Q), :] = unpacked_quarter(refs[n][b, j].astype(F32)).astype(BF16)
            return _

        lax.fori_loop(0, 32, piece, 0)


def unpack(at, groups):
    group = (4, 8, QP, 128)
    return pl.pallas_call(
        unpack_kernel,
        grid_spec=pltpu.PrefetchScalarGridSpec(
            num_scalar_prefetch=1,
            grid=(1,),
            in_specs=[whole(group)] * 8,
            out_specs=whole((64, R, R)),
        ),
        out_shape=jax.ShapeDtypeStruct((64, R, R), BF16),
        cost_estimate=pl.CostEstimate(
            flops=64 * 4 * R * R, transcendentals=0, bytes_accessed=64 * 4 * R * R
        ),
        name="unpack",
    )(at, *groups)


def local_kernel(ends_ref, rank_ref, p_ref, m_ref, v_ref, x_ref, own_ref, base_ref):
    step = pl.program_id(0)
    for i in range(STEP):
        pair = step * STEP + i
        inside = masks((rank_ref[pair] + 1) * RSTEP)
        own = dot(p_ref[i], x_ref[ends_ref[pair * 2]], ((1,), (0,)))
        own = own + dot(p_ref[i], x_ref[ends_ref[pair * 2 + 1]], ((1,), (0,)))
        for q in range(4):
            own_ref[i, q] = packed_quarter(own, q).astype(BF16)
        masked = jnp.where(inside, m_ref[i].astype(F32), 0.0).astype(BF16)
        base_ref[i] = v_ref[i].astype(F32) + dot(masked, v_ref[i], ((1,), (0,)))


def local(ends, rank, p, m, v, blocks):
    pairs = p.shape[0]
    block = pl.BlockSpec((STEP, R, R), lambda i, *_: (i, 0, 0))
    return pl.pallas_call(
        local_kernel,
        grid_spec=pltpu.PrefetchScalarGridSpec(
            num_scalar_prefetch=2,
            grid=(pairs // STEP,),
            in_specs=[block, block, block, whole((64, R, R))],
            out_specs=[pl.BlockSpec((STEP, 4, QP, 128), lambda i, *_: (i, 0, 0, 0)), block],
        ),
        out_shape=[
            jax.ShapeDtypeStruct((pairs, 4, QP, 128), BF16),
            jax.ShapeDtypeStruct((pairs, R, R), F32),
        ],
        cost_estimate=pl.CostEstimate(
            flops=pairs * 6 * R**3, transcendentals=0, bytes_accessed=pairs * 12 * R * R
        ),
        name="local",
    )(ends, rank, p, m, v, blocks)


def couple_kernel(at_ref, d0_ref, d1_ref, d2_ref, d3_ref, x_ref, c_ref):
    total = d0_ref[0].astype(F32) + d1_ref[0].astype(F32)
    total = total + (d2_ref[0].astype(F32) + d3_ref[0].astype(F32))
    domain = unpacked_quarter(total).astype(BF16)
    coupled = dot(domain, x_ref[0], ((1,), (0,)))
    c_ref[0] = packed_quarter(coupled, 0).astype(BF16)


def couple(at, parts, blocks):
    def orbital(t, at_ref):
        return ((at_ref[0] * 2 + at_ref[1]) * 8 + (at_ref[2] ^ (2 * t)), 0, 0)

    return pl.pallas_call(
        couple_kernel,
        grid_spec=pltpu.PrefetchScalarGridSpec(
            num_scalar_prefetch=1,
            grid=(4,),
            in_specs=[
                pl.BlockSpec((1, QP, 128), lambda t, at_ref, d=d: (t ^ d, 0, 0)) for d in range(4)
            ]
            + [pl.BlockSpec((1, R, R), orbital)],
            out_specs=pl.BlockSpec((1, QP, 128), lambda t, at_ref: (t, 0, 0)),
        ),
        out_shape=jax.ShapeDtypeStruct((4, QP, 128), BF16),
        cost_estimate=pl.CostEstimate(
            flops=8 * Q * R * R, transcendentals=0, bytes_accessed=16 * R * R
        ),
        name="couple",
    )(at, *parts, blocks)


def finish_kernel(ends_ref, rank_ref, at_ref, s_ref, own_ref, base_ref, *rest):
    group_refs, out_ref, held_ref, sem = rest[:8], rest[8], rest[9], rest[10]
    step = pl.program_id(0)

    @pl.when(step == 0)
    def _():
        copies = [
            pltpu.make_async_copy(group_refs[n], held_ref.at[pl.ds(n * 32, 32)], sem.at[n])
            for n in range(8)
        ]
        for copy in copies:
            copy.start()
        for copy in copies:
            copy.wait()

    for i in range(STEP):
        pair = step * STEP + i
        quarters = []
        for q in range(4):
            first = held_ref[slot_of(ends_ref[pair * 2], q, at_ref)].astype(F32)
            second = held_ref[slot_of(ends_ref[pair * 2 + 1], q, at_ref)].astype(F32)
            quarters.append(unpacked_quarter((first + second) - own_ref[i, q].astype(F32)))
        combined = jnp.concatenate(quarters, axis=0).astype(BF16)
        half = dot(s_ref[i], combined, ((0,), (0,))).astype(BF16)
        total = base_ref[i] + dot(half, s_ref[i], ((1,), (0,)))
        inside = masks((rank_ref[pair] + 1) * RSTEP)
        out_ref[i] = jnp.where(inside, total, 0.0).astype(BF16)


def finish(ends, rank, at, s, own, base, groups):
    pairs = s.shape[0]
    block = pl.BlockSpec((STEP, R, R), lambda i, *_: (i, 0, 0))
    return pl.pallas_call(
        finish_kernel,
        grid_spec=pltpu.PrefetchScalarGridSpec(
            num_scalar_prefetch=3,
            grid=(pairs // STEP,),
            in_specs=[block, pl.BlockSpec((STEP, 4, QP, 128), lambda i, *_: (i, 0, 0, 0)), block]
            + [pl.BlockSpec(memory_space=pltpu.HBM)] * 8,
            out_specs=block,
            scratch_shapes=[pltpu.VMEM((256, QP, 128), BF16), pltpu.SemaphoreType.DMA((8,))],
        ),
        out_shape=jax.ShapeDtypeStruct((pairs, R, R), BF16),
        cost_estimate=pl.CostEstimate(
            flops=pairs * 4 * R**3, transcendentals=0, bytes_accessed=pairs * 10 * R * R
        ),
        name="finish",
    )(ends, rank, at, s, own, base, *[g.reshape(32, QP, 128) for g in groups])


def added(*arrays):
    total = arrays[0].astype(F32)
    for a in arrays[1:]:
        total = total + a.astype(F32)
    return total.astype(BF16)


def sent_to_all(mine):
    both = jnp.concatenate([mine, stage_z(mine, 1)], axis=0)
    group = jnp.stack([both] + [stage_b(both, d) for d in (1, 2, 3)], axis=0)
    groups = [group] + [stage_a(group, d) for d in (1, 2, 3)]
    return groups + [stage_c(g) for g in groups]


def body(pair_list, rank_bucket, amplitudes, intersects, integrals, exchange_blocks):
    pairs = amplitudes.shape[0]
    at = jnp.stack([lax.axis_index(a) for a in AXES]).astype(jnp.int32)
    y = lax.axis_index("gz")
    ends = pair_list.reshape(pairs * 2)
    s = intersects.reshape(pairs, R, R)
    m = amplitudes.reshape(pairs, R, R)
    v = integrals.reshape(pairs, R, R)

    quarter = lax.dynamic_slice_in_dim(exchange_blocks.reshape(R, R), y * Q, Q, axis=0)
    quarter = packed_quarter(quarter, 0)
    near = [quarter] + [stage_z(quarter, 2 * d) for d in (1, 2, 3)]
    blocks = unpack(at, sent_to_all(jnp.stack(near, axis=0)))

    p, *sums = project(ends, rank_bucket, at, s, m)
    sums = [added(sums[a], stage_c(sums[4 + a])) for a in range(4)]
    sums = added(sums[0], *[stage_a(sums[d], d) for d in (1, 2, 3)])
    sums = added(sums[0], *[stage_b(sums[d], d) for d in (1, 2, 3)])
    sums = added(sums[:4], stage_z(sums[4:], 1))
    parts = [sums] + [stage_z(sums, 2 * d) for d in (1, 2, 3)]
    own, base = local(ends, rank_bucket, p, m, v, blocks)
    groups = sent_to_all(couple(at, parts, blocks))
    out = finish(ends, rank_bucket, at, s, own, base, groups)
    return out.reshape(pairs, R * R)


def solution(mesh):
    torus = Mesh(mesh.devices.reshape(4, 2, mesh.shape["gy"], mesh.shape["gz"]), AXES)
    everywhere = P(AXES, None)
    return jax.shard_map(
        body,
        mesh=torus,
        in_specs=(everywhere, P(AXES), everywhere, everywhere, everywhere, P(GX_GY, None)),
        out_specs=everywhere,
        check_vma=False,
    )
```

```python
import jax
import jax.numpy as jnp
from jax import lax
from jax.experimental import pallas as pl
from jax.experimental.pallas import tpu as pltpu
from jax.sharding import Mesh
from jax.sharding import PartitionSpec as P

RSTEP = 64
R = 192
Q = 48
QP = 72
STEP = 8
AXES = ("gx_0", "gx_1", "gy", "gz")
GX_GY = ("gx_0", "gx_1", "gy")
BF16 = jnp.bfloat16
F32 = jnp.float32


def device_number(x, c, z, y):
    return ((x * 2 + c) * 8 + z) * 4 + y


def pairs_of(move):
    out = []
    for x in range(4):
        for c in range(2):
            for z in range(8):
                for y in range(4):
                    out.append((device_number(x, c, z, y), device_number(*move(x, c, z, y))))
    return out


def stage_a(array, d):
    return lax.ppermute(
        array, AXES, pairs_of(lambda x, c, z, y: (x ^ d, c, z, y) if c == 0 else (x, c, z, y ^ d))
    )


def stage_b(array, d):
    return lax.ppermute(
        array, AXES, pairs_of(lambda x, c, z, y: (x, c, z, y ^ d) if c == 0 else (x ^ d, c, z, y))
    )


def stage_z(array, d):
    return lax.ppermute(array, AXES, pairs_of(lambda x, c, z, y: (x, c, z ^ d, y)))


def stage_c(array):
    return lax.ppermute(array, AXES, pairs_of(lambda x, c, z, y: (x, c ^ 1, z, y)))


def slot_of(k, q, at_ref):
    x, c, z, y = (at_ref[i] for i in range(4))
    core = (k >> 3) & 1
    dx, dq, dz = (k >> 4) ^ x, q ^ y, (k & 7) ^ z
    a = jnp.where(core == 0, dx, dq)
    b = jnp.where(core == 0, dq, dx)
    return (((core ^ c) * 4 + a) * 4 + b) * 8 + (dz & 1) * 4 + (dz >> 1)


def packed_quarter(block, q):
    rows = block[q * Q : (q + 1) * Q]
    right = jnp.concatenate([rows[: Q // 2, 128:], rows[Q // 2 :, 128:]], axis=1)
    return jnp.concatenate([rows[:, :128], right], axis=0)


def unpacked_quarter(piece):
    right = piece[Q:]
    right = jnp.concatenate([right[:, :64], right[:, 64:]], axis=0)
    return jnp.concatenate([piece[:Q], right], axis=1)


def masks(rank):
    rows = lax.broadcasted_iota(jnp.int32, (R, R), 0)
    cols = lax.broadcasted_iota(jnp.int32, (R, R), 1)
    return (rows < rank) & (cols < rank)


def dot(a, b, dims):
    return lax.dot_general(a, b, (dims, ((), ())), preferred_element_type=F32)


VLIM = 20

SMEM = pl.BlockSpec(memory_space=pltpu.SMEM)
VMEM = pl.BlockSpec(memory_space=pltpu.VMEM)
GROUP = (4, 8, QP, 128)


def call(kernel, n_smem, n_vmem, out_shape, scratch, flops, limit_mib):
    return pl.pallas_call(
        kernel,
        in_specs=[SMEM] * n_smem + [VMEM] * n_vmem,
        out_specs=jax.tree.map(lambda _: VMEM, out_shape),
        out_shape=out_shape,
        scratch_shapes=scratch,
        compiler_params=pltpu.CompilerParams(vmem_limit_bytes=limit_mib << 20),
        cost_estimate=pl.CostEstimate(flops=flops, transcendentals=0, bytes_accessed=1 << 20),
    )


def each_pair(pairs, work):
    def step(n, _):
        for i in range(STEP):
            work(n * STEP + i)
        return _

    lax.fori_loop(0, pairs // STEP, step, 0)


def project_kernel(ends_ref, rank_ref, at_ref, s_ref, m_ref, p_ref, *rest):
    out_refs, sums_ref = rest[:8], rest[8]
    sums_ref[...] = jnp.zeros_like(sums_ref)

    def work(pair):
        inside = masks((rank_ref[pair] + 1) * RSTEP)
        masked = jnp.where(inside, m_ref[pair].astype(F32), 0.0).astype(BF16)
        half = dot(s_ref[pair], masked, ((1,), (0,))).astype(BF16)
        full = dot(half, s_ref[pair], ((1,), (1,)))
        p_ref[pair] = full.astype(BF16)
        for q in range(4):
            piece = packed_quarter(full, q).astype(BF16)
            for e in range(2):
                slot = slot_of(ends_ref[e, pair], q, at_ref)
                sums_ref[slot] = sums_ref[slot] + piece

    each_pair(s_ref.shape[0], work)
    for n in range(8):
        out_refs[n][...] = sums_ref[n * 32 : (n + 1) * 32].reshape(GROUP)


def project(ends, rank, at, s, m):
    pairs = s.shape[0]
    return call(
        project_kernel,
        3,
        2,
        [jax.ShapeDtypeStruct((pairs, R, R), BF16)] + [jax.ShapeDtypeStruct(GROUP, BF16)] * 8,
        [pltpu.VMEM((256, QP, 128), BF16)],
        pairs * 4 * R**3,
        VLIM,
    )(ends, rank, at, s, m)


def base_kernel(rank_ref, m_ref, v_ref, base_ref):
    def work(pair):
        inside = masks((rank_ref[pair] + 1) * RSTEP)
        masked = jnp.where(inside, m_ref[pair].astype(F32), 0.0).astype(BF16)
        base_ref[pair] = v_ref[pair].astype(F32) + dot(masked, v_ref[pair], ((1,), (0,)))

    each_pair(m_ref.shape[0], work)


def base_of(rank, m, v):
    pairs = m.shape[0]
    return call(
        base_kernel, 1, 2, jax.ShapeDtypeStruct((pairs, R, R), F32), [], pairs * 2 * R**3, VLIM
    )(rank, m, v)


def own_kernel(ends_ref, at_ref, p_ref, *rest):
    group_refs, own_ref, held_ref = rest[:8], rest[8], rest[9]
    for n in range(8):
        held_ref[n * 32 : (n + 1) * 32] = group_refs[n][...].reshape(32, QP, 128)

    def work(pair):
        quarters = []
        for q in range(4):
            first = held_ref[slot_of(ends_ref[0, pair], q, at_ref)].astype(F32)
            second = held_ref[slot_of(ends_ref[1, pair], q, at_ref)].astype(F32)
            quarters.append(unpacked_quarter(first + second))
        both = jnp.concatenate(quarters, axis=0).astype(BF16)
        own = dot(p_ref[pair], both, ((1,), (0,)))
        for q in range(4):
            own_ref[pair, q] = packed_quarter(own, q).astype(BF16)

    each_pair(p_ref.shape[0], work)


def own_of(ends, at, p, groups):
    pairs = p.shape[0]
    return call(
        own_kernel,
        2,
        9,
        jax.ShapeDtypeStruct((pairs, 4, QP, 128), BF16),
        [pltpu.VMEM((256, QP, 128), BF16)],
        pairs * 2 * R**3,
        VLIM,
    )(ends, at, p, *groups)


def couple_kernel(d0_ref, d1_ref, d2_ref, d3_ref, x0_ref, x1_ref, x2_ref, x3_ref, c_ref):
    for t, x_ref in enumerate((x0_ref, x1_ref, x2_ref, x3_ref)):
        total = d0_ref[t].astype(F32) + d1_ref[t ^ 1].astype(F32)
        total = total + (d2_ref[t ^ 2].astype(F32) + d3_ref[t ^ 3].astype(F32))
        domain = unpacked_quarter(total).astype(BF16)
        block = [unpacked_quarter(x_ref[q].astype(F32)) for q in range(4)]
        block = jnp.concatenate(block, axis=0).astype(BF16)
        c_ref[t] = packed_quarter(dot(domain, block, ((1,), (0,))), 0).astype(BF16)


def couple(parts, near):
    return call(
        couple_kernel, 0, 8, jax.ShapeDtypeStruct((4, QP, 128), BF16), [], 8 * Q * R * R, VLIM
    )(*parts, *near)


def finish_kernel(ends_ref, rank_ref, at_ref, s_ref, own_ref, base_ref, *rest):
    group_refs, out_ref, held_ref = rest[:8], rest[8], rest[9]
    for n in range(8):
        held_ref[n * 32 : (n + 1) * 32] = group_refs[n][...].reshape(32, QP, 128)

    def work(pair):
        quarters = []
        for q in range(4):
            first = held_ref[slot_of(ends_ref[0, pair], q, at_ref)].astype(F32)
            second = held_ref[slot_of(ends_ref[1, pair], q, at_ref)].astype(F32)
            quarters.append(unpacked_quarter((first + second) - own_ref[pair, q].astype(F32)))
        combined = jnp.concatenate(quarters, axis=0).astype(BF16)
        half = dot(s_ref[pair], combined, ((0,), (0,))).astype(BF16)
        total = base_ref[pair] + dot(half, s_ref[pair], ((1,), (0,)))
        inside = masks((rank_ref[pair] + 1) * RSTEP)
        out_ref[pair] = jnp.where(inside, total, 0.0).astype(BF16)

    each_pair(s_ref.shape[0], work)


def finish(ends, rank, at, s, own, base, groups):
    pairs = s.shape[0]
    return call(
        finish_kernel,
        3,
        11,
        jax.ShapeDtypeStruct((pairs, R, R), BF16),
        [pltpu.VMEM((256, QP, 128), BF16)],
        pairs * 4 * R**3,
        VLIM,
    )(ends, rank, at, s, own, base, *groups)


def added(*arrays):
    total = arrays[0].astype(F32)
    for a in arrays[1:]:
        total = total + a.astype(F32)
    return total.astype(BF16)


def sent_to_all(mine):
    both = jnp.concatenate([mine, stage_z(mine, 1)], axis=0)
    group = [both] + [stage_b(both, d) for d in (1, 2, 3)]
    group = jnp.stack(group, axis=0)
    groups = [group] + [stage_a(group, d) for d in (2, 1, 3)]
    groups = [groups[0], groups[2], groups[1], groups[3]]
    return groups + [stage_c(groups[n]) for n in range(4)]


def whole_step(pair_list, rank_bucket, amplitudes, intersects, integrals, exchange_blocks):
    pairs = amplitudes.shape[0]
    at = jnp.stack([lax.axis_index(a) for a in AXES]).astype(jnp.int32)
    y = lax.axis_index("gz")
    ends = pair_list.T

    block = exchange_blocks.reshape(R, R)
    block = jnp.stack([packed_quarter(block, q) for q in range(4)], axis=0)
    near = [block] + [stage_z(block, 2 * d) for d in (1, 2, 3)]
    quarters = [lax.dynamic_slice_in_dim(b, y, 1, axis=0) for b in near]
    quarters = jnp.concatenate(quarters, axis=0)
    blocks = sent_to_all(quarters)

    m = amplitudes.reshape(pairs, R, R)
    s = intersects.reshape(pairs, R, R)
    p, *sums = project(ends, rank_bucket, at, s, m)
    v = integrals.reshape(pairs, R, R)
    base = base_of(rank_bucket, m, v)

    sums = [added(sums[a], stage_c(sums[4 + a])) for a in (2, 1, 3, 0)]
    moved = [stage_a(sums[n], d) for n, d in enumerate((2, 1, 3))]
    sums = added(sums[3], *moved)
    sums = added(sums[0], *[stage_b(sums[d], d) for d in (1, 2, 3)])
    sums = added(sums[:4], stage_z(sums[4:], 1))
    parts = [sums] + [stage_z(sums, 2 * d) for d in (1, 2, 3)]
    coupled = couple(parts, near)
    own = own_of(ends, at, p, blocks)
    groups = sent_to_all(coupled)
    out = finish(ends, rank_bucket, at, s, own, base, groups)
    return out.reshape(pairs, R * R)


def solution(mesh):
    torus = Mesh(mesh.devices.reshape(4, 2, mesh.shape["gy"], mesh.shape["gz"]), AXES)
    everywhere = P(AXES, None)
    return jax.shard_map(
        whole_step,
        mesh=torus,
        in_specs=(everywhere, P(AXES), everywhere, everywhere, everywhere, P(GX_GY, None)),
        out_specs=everywhere,
        check_vma=False,
    )
```

```python
import jax
import jax.numpy as jnp
from jax import lax
from jax.experimental import pallas as pl
from jax.experimental.pallas import tpu as pltpu
from jax.sharding import Mesh
from jax.sharding import PartitionSpec as P

RSTEP = 64
R = 192
Q = 48
QP = 72
CHUNKS = R * R // 128
STEP = 8
AXES = ("gx_0", "gx_1", "gy", "gz")
GX_GY = ("gx_0", "gx_1", "gy")
BF16 = jnp.bfloat16
F32 = jnp.float32


def device_number(x, c, z, y):
    return ((x * 2 + c) * 8 + z) * 4 + y


def pairs_of(move):
    out = []
    for x in range(4):
        for c in range(2):
            for z in range(8):
                for y in range(4):
                    out.append((device_number(x, c, z, y), device_number(*move(x, c, z, y))))
    return out


def stage_a(array, d):
    return lax.ppermute(
        array, AXES, pairs_of(lambda x, c, z, y: (x ^ d, c, z, y) if c == 0 else (x, c, z, y ^ d))
    )


def stage_b(array, d):
    return lax.ppermute(
        array, AXES, pairs_of(lambda x, c, z, y: (x, c, z, y ^ d) if c == 0 else (x ^ d, c, z, y))
    )


def stage_z(array, d):
    return lax.ppermute(array, AXES, pairs_of(lambda x, c, z, y: (x, c, z ^ d, y)))


def stage_c(array):
    return lax.ppermute(array, AXES, pairs_of(lambda x, c, z, y: (x, c ^ 1, z, y)))


def slot_of(k, q, at_ref):
    x, c, z, y = (at_ref[i] for i in range(4))
    core = (k >> 3) & 1
    dx, dq, dz = (k >> 4) ^ x, q ^ y, (k & 7) ^ z
    a = jnp.where(core == 0, dx, dq)
    b = jnp.where(core == 0, dq, dx)
    return (((core ^ c) * 4 + a) * 4 + b) * 8 + (dz & 1) * 4 + (dz >> 1)


def packed_quarter(block, q):
    rows = block[q * Q : (q + 1) * Q]
    right = jnp.concatenate([rows[: Q // 2, 128:], rows[Q // 2 :, 128:]], axis=1)
    return jnp.concatenate([rows[:, :128], right], axis=0)


def unpacked_quarter(piece):
    right = piece[Q:]
    right = jnp.concatenate([right[:, :64], right[:, 64:]], axis=0)
    return jnp.concatenate([piece[:Q], right], axis=1)


def masks(rank):
    rows = lax.broadcasted_iota(jnp.int32, (R, R), 0)
    cols = lax.broadcasted_iota(jnp.int32, (R, R), 1)
    return (rows < rank) & (cols < rank)


def dot(a, b, dims):
    return lax.dot_general(a, b, (dims, ((), ())), preferred_element_type=F32)


VLIM = 14

SMEM = pl.BlockSpec(memory_space=pltpu.SMEM)
VMEM = pl.BlockSpec(memory_space=pltpu.VMEM)
GROUP = (4, 8, QP, 128)


def call(kernel, n_smem, n_vmem, out_shape, scratch, flops, limit_mib):
    return pl.pallas_call(
        kernel,
        in_specs=[SMEM] * n_smem + [VMEM] * n_vmem,
        out_specs=jax.tree.map(lambda _: VMEM, out_shape),
        out_shape=out_shape,
        scratch_shapes=scratch,
        compiler_params=pltpu.CompilerParams(vmem_limit_bytes=limit_mib << 20),
        cost_estimate=pl.CostEstimate(flops=flops, transcendentals=0, bytes_accessed=1 << 20),
    )


def each_pair(pairs, work):
    def step(n, _):
        for i in range(STEP):
            work(n * STEP + i)
        return _

    lax.fori_loop(0, pairs // STEP, step, 0)


def relay_kernel(x_ref, o_ref, flat_ref, left_ref, right_ref):
    low = lax.broadcasted_iota(jnp.int32, (R // 2, 128), 1) < 64

    def work(g, _):
        rows = pl.ds(pl.multiple_of(g * 8, 8), 8)
        for j in range(CHUNKS):
            flat_ref[j * 8 : j * 8 + 8] = x_ref[rows, j * 128 : j * 128 + 128].astype(F32)
        for i in range(8):
            first, second, third = (
                flat_ref[pl.ds(n * 8 + i, R // 2, stride=24), :] for n in range(3)
            )
            second_turned, third_turned = pltpu.roll(second, 64, 1), pltpu.roll(third, 64, 1)
            left_ref[i, pl.ds(0, R // 2, stride=2), :] = first
            right_ref[i, pl.ds(0, R // 2, stride=2), :] = second
            left_ref[i, pl.ds(1, R // 2, stride=2), :] = jnp.where(low, second_turned, third_turned)
            right_ref[i, pl.ds(1, R // 2, stride=2), :] = third_turned
            o_ref[g * 8 + i, :, :128] = left_ref[i].astype(BF16)
            o_ref[g * 8 + i, :, 128:] = right_ref[i][:, :64].astype(BF16)
        return _

    lax.fori_loop(0, x_ref.shape[0] // 8, work, 0)


def relay(x):
    pairs = x.shape[0]
    return call(
        relay_kernel,
        0,
        1,
        jax.ShapeDtypeStruct((pairs, R, R), BF16),
        [
            pltpu.VMEM((CHUNKS * 8, 128), F32),
            pltpu.VMEM((8, R, 128), F32),
            pltpu.VMEM((8, R, 128), F32),
        ],
        1 << 24,
        VLIM,
    )(x)


def lay_out(block, i, flat_ref, left_ref, right_ref):
    low = lax.broadcasted_iota(jnp.int32, (R // 2, 128), 1) < 64
    left_ref[i] = block[:, :128]
    right_ref[i, :, :64] = block[:, 128:]
    even = pl.ds(0, R // 2, stride=2)
    odd = pl.ds(1, R // 2, stride=2)
    turned = pltpu.roll(left_ref[i, odd, :], 64, 1)
    flat_ref[pl.ds(i, R // 2, stride=24), :] = left_ref[i, even, :]
    flat_ref[pl.ds(8 + i, R // 2, stride=24), :] = jnp.where(low, right_ref[i, even, :], turned)
    flat_ref[pl.ds(16 + i, R // 2, stride=24), :] = jnp.where(
        low, turned, pltpu.roll(right_ref[i, odd, :], 64, 1)
    )


def project_kernel(ends_ref, rank_ref, at_ref, s_ref, m_ref, p_ref, *rest):
    out_refs, sums_ref = rest[:8], rest[8]
    sums_ref[...] = jnp.zeros_like(sums_ref)

    def work(pair):
        inside = masks((rank_ref[pair] + 1) * RSTEP)
        masked = jnp.where(inside, m_ref[pair].astype(F32), 0.0).astype(BF16)
        half = dot(s_ref[pair], masked, ((1,), (0,))).astype(BF16)
        full = dot(half, s_ref[pair], ((1,), (1,)))
        p_ref[pair] = full.astype(BF16)
        for q in range(4):
            piece = packed_quarter(full, q).astype(BF16)
            for e in range(2):
                slot = slot_of(ends_ref[e, pair], q, at_ref)
                sums_ref[slot] = sums_ref[slot] + piece

    each_pair(s_ref.shape[0], work)
    for n in range(8):
        out_refs[n][...] = sums_ref[n * 32 : (n + 1) * 32].reshape(GROUP)


def project(ends, rank, at, s, m):
    pairs = s.shape[0]
    return call(
        project_kernel,
        3,
        2,
        [jax.ShapeDtypeStruct((pairs, R, R), BF16)] + [jax.ShapeDtypeStruct(GROUP, BF16)] * 8,
        [pltpu.VMEM((256, QP, 128), BF16)],
        pairs * 4 * R**3,
        VLIM,
    )(ends, rank, at, s, m)


def base_kernel(rank_ref, m_ref, v_ref, base_ref):
    def work(pair):
        inside = masks((rank_ref[pair] + 1) * RSTEP)
        masked = jnp.where(inside, m_ref[pair].astype(F32), 0.0).astype(BF16)
        base_ref[pair] = v_ref[pair].astype(F32) + dot(masked, v_ref[pair], ((1,), (0,)))

    each_pair(m_ref.shape[0], work)


def base_of(rank, m, v):
    pairs = m.shape[0]
    return call(
        base_kernel, 1, 2, jax.ShapeDtypeStruct((pairs, R, R), F32), [], pairs * 2 * R**3, VLIM
    )(rank, m, v)


def own_kernel(ends_ref, at_ref, p_ref, *rest):
    group_refs, own_ref, held_ref = rest[:8], rest[8], rest[9]
    for n in range(8):
        held_ref[n * 32 : (n + 1) * 32] = group_refs[n][...].reshape(32, QP, 128)

    def work(pair):
        quarters = []
        for q in range(4):
            first = held_ref[slot_of(ends_ref[0, pair], q, at_ref)].astype(F32)
            second = held_ref[slot_of(ends_ref[1, pair], q, at_ref)].astype(F32)
            quarters.append(unpacked_quarter(first + second))
        both = jnp.concatenate(quarters, axis=0).astype(BF16)
        own = dot(p_ref[pair], both, ((1,), (0,)))
        for q in range(4):
            own_ref[pair, q] = packed_quarter(own, q).astype(BF16)

    each_pair(p_ref.shape[0], work)


def own_of(ends, at, p, groups):
    pairs = p.shape[0]
    return call(
        own_kernel,
        2,
        9,
        jax.ShapeDtypeStruct((pairs, 4, QP, 128), BF16),
        [pltpu.VMEM((256, QP, 128), BF16)],
        pairs * 2 * R**3,
        VLIM,
    )(ends, at, p, *groups)


def couple_kernel(d0_ref, d1_ref, d2_ref, d3_ref, x0_ref, x1_ref, x2_ref, x3_ref, c_ref):
    for t, x_ref in enumerate((x0_ref, x1_ref, x2_ref, x3_ref)):
        total = d0_ref[t].astype(F32) + d1_ref[t ^ 1].astype(F32)
        total = total + (d2_ref[t ^ 2].astype(F32) + d3_ref[t ^ 3].astype(F32))
        domain = unpacked_quarter(total).astype(BF16)
        block = [unpacked_quarter(x_ref[q].astype(F32)) for q in range(4)]
        block = jnp.concatenate(block, axis=0).astype(BF16)
        c_ref[t] = packed_quarter(dot(domain, block, ((1,), (0,))), 0).astype(BF16)


def couple(parts, near):
    return call(
        couple_kernel, 0, 8, jax.ShapeDtypeStruct((4, QP, 128), BF16), [], 8 * Q * R * R, VLIM
    )(*parts, *near)


def finish_kernel(ends_ref, rank_ref, at_ref, s_ref, own_ref, base_ref, *rest):
    group_refs, out_ref, held_ref = rest[:8], rest[8], rest[9]
    flat_ref, left_ref, right_ref = rest[10:]
    for n in range(8):
        held_ref[n * 32 : (n + 1) * 32] = group_refs[n][...].reshape(32, QP, 128)
    right_ref[...] = jnp.zeros_like(right_ref)

    def work(g, _):
        for i in range(8):
            pair = g * 8 + i
            quarters = []
            for q in range(4):
                first = held_ref[slot_of(ends_ref[0, pair], q, at_ref)].astype(F32)
                second = held_ref[slot_of(ends_ref[1, pair], q, at_ref)].astype(F32)
                quarters.append(unpacked_quarter((first + second) - own_ref[pair, q].astype(F32)))
            combined = jnp.concatenate(quarters, axis=0).astype(BF16)
            half = dot(s_ref[pair], combined, ((0,), (0,))).astype(BF16)
            total = base_ref[pair] + dot(half, s_ref[pair], ((1,), (0,)))
            inside = masks((rank_ref[pair] + 1) * RSTEP)
            lay_out(jnp.where(inside, total, 0.0), i, flat_ref, left_ref, right_ref)
        rows = pl.ds(pl.multiple_of(g * 8, 8), 8)
        for j in range(CHUNKS):
            out_ref[rows, j * 128 : j * 128 + 128] = flat_ref[j * 8 : j * 8 + 8].astype(BF16)
        return _

    lax.fori_loop(0, s_ref.shape[0] // 8, work, 0)


def finish(ends, rank, at, s, own, base, groups):
    pairs = s.shape[0]
    return call(
        finish_kernel,
        3,
        11,
        jax.ShapeDtypeStruct((pairs, R * R), BF16),
        [
            pltpu.VMEM((256, QP, 128), BF16),
            pltpu.VMEM((CHUNKS * 8, 128), F32),
            pltpu.VMEM((8, R, 128), F32),
            pltpu.VMEM((8, R, 128), F32),
        ],
        pairs * 4 * R**3,
        VLIM,
    )(ends, rank, at, s, own, base, *groups)


def added(*arrays):
    total = arrays[0].astype(F32)
    for a in arrays[1:]:
        total = total + a.astype(F32)
    return total.astype(BF16)


def sent_to_all(mine):
    both = jnp.concatenate([mine, stage_z(mine, 1)], axis=0)
    group = [both] + [stage_b(both, d) for d in (1, 2, 3)]
    group = jnp.stack(group, axis=0)
    groups = [group] + [stage_a(group, d) for d in (2, 1, 3)]
    groups = [groups[0], groups[2], groups[1], groups[3]]
    return groups + [stage_c(groups[n]) for n in range(4)]


def whole_step(pair_list, rank_bucket, amplitudes, intersects, integrals, exchange_blocks):
    at = jnp.stack([lax.axis_index(a) for a in AXES]).astype(jnp.int32)
    y = lax.axis_index("gz")
    ends = pair_list.T

    block = exchange_blocks.reshape(R, R)
    block = jnp.stack([packed_quarter(block, q) for q in range(4)], axis=0)
    near = [block] + [stage_z(block, 2 * d) for d in (1, 2, 3)]
    quarters = [lax.dynamic_slice_in_dim(b, y, 1, axis=0) for b in near]
    quarters = jnp.concatenate(quarters, axis=0)
    blocks = sent_to_all(quarters)

    m = relay(amplitudes)
    s = relay(intersects)
    p, *sums = project(ends, rank_bucket, at, s, m)
    v = relay(integrals)
    base = base_of(rank_bucket, m, v)

    sums = [added(sums[a], stage_c(sums[4 + a])) for a in (2, 1, 3, 0)]
    moved = [stage_a(sums[n], d) for n, d in enumerate((2, 1, 3))]
    sums = added(sums[3], *moved)
    sums = added(sums[0], *[stage_b(sums[d], d) for d in (1, 2, 3)])
    sums = added(sums[:4], stage_z(sums[4:], 1))
    parts = [sums] + [stage_z(sums, 2 * d) for d in (1, 2, 3)]
    coupled = couple(parts, near)
    own = own_of(ends, at, p, blocks)
    groups = sent_to_all(coupled)
    return finish(ends, rank_bucket, at, s, own, base, groups)


def solution(mesh):
    torus = Mesh(mesh.devices.reshape(4, 2, mesh.shape["gy"], mesh.shape["gz"]), AXES)
    everywhere = P(AXES, None)
    return jax.shard_map(
        whole_step,
        mesh=torus,
        in_specs=(everywhere, P(AXES), everywhere, everywhere, everywhere, P(GX_GY, None)),
        out_specs=everywhere,
        check_vma=False,
    )
```

```python
import jax
import jax.numpy as jnp
from jax import lax
from jax.experimental import pallas as pl
from jax.experimental.pallas import tpu as pltpu
from jax.sharding import Mesh
from jax.sharding import PartitionSpec as P

RSTEP = 64
R = 192
Q = 48
QP = 72
CHUNKS = R * R // 128
STEP = 8
AXES = ("gx_0", "gx_1", "gy", "gz")
GX_GY = ("gx_0", "gx_1", "gy")
BF16 = jnp.bfloat16
F32 = jnp.float32


def device_number(x, c, z, y):
    return ((x * 2 + c) * 8 + z) * 4 + y


def pairs_of(move):
    out = []
    for x in range(4):
        for c in range(2):
            for z in range(8):
                for y in range(4):
                    out.append((device_number(x, c, z, y), device_number(*move(x, c, z, y))))
    return out


def stage_a(array, d):
    return lax.ppermute(
        array, AXES, pairs_of(lambda x, c, z, y: (x ^ d, c, z, y) if c == 0 else (x, c, z, y ^ d))
    )


def stage_b(array, d):
    return lax.ppermute(
        array, AXES, pairs_of(lambda x, c, z, y: (x, c, z, y ^ d) if c == 0 else (x ^ d, c, z, y))
    )


def stage_z(array, d):
    return lax.ppermute(array, AXES, pairs_of(lambda x, c, z, y: (x, c, z ^ d, y)))


def stage_c(array):
    return lax.ppermute(array, AXES, pairs_of(lambda x, c, z, y: (x, c ^ 1, z, y)))


def slot_of(k, q, at_ref):
    x, c, z, y = (at_ref[i] for i in range(4))
    core = (k >> 3) & 1
    dx, dq, dz = (k >> 4) ^ x, q ^ y, (k & 7) ^ z
    a = jnp.where(core == 0, dx, dq)
    b = jnp.where(core == 0, dq, dx)
    return (((core ^ c) * 4 + a) * 4 + b) * 8 + (dz & 1) * 4 + (dz >> 1)


def packed_quarter(block, q):
    rows = block[q * Q : (q + 1) * Q]
    right = jnp.concatenate([rows[: Q // 2, 128:], rows[Q // 2 :, 128:]], axis=1)
    return jnp.concatenate([rows[:, :128], right], axis=0)


def unpacked_quarter(piece):
    right = piece[Q:]
    right = jnp.concatenate([right[:, :64], right[:, 64:]], axis=0)
    return jnp.concatenate([piece[:Q], right], axis=1)


def masks(rank):
    rows = lax.broadcasted_iota(jnp.int32, (R, R), 0)
    cols = lax.broadcasted_iota(jnp.int32, (R, R), 1)
    return (rows < rank) & (cols < rank)


def dot(a, b, dims):
    return lax.dot_general(a, b, (dims, ((), ())), preferred_element_type=F32)


VLIM = 14

SMEM = pl.BlockSpec(memory_space=pltpu.SMEM)
VMEM = pl.BlockSpec(memory_space=pltpu.VMEM)
HBM = pl.BlockSpec(memory_space=pltpu.HBM)
GROUP = (4, 8, QP, 128)


def call(kernel, in_specs, out_shape, out_specs, scratch, flops):
    return pl.pallas_call(
        kernel,
        in_specs=in_specs,
        out_specs=out_specs,
        out_shape=out_shape,
        scratch_shapes=scratch,
        compiler_params=pltpu.CompilerParams(vmem_limit_bytes=VLIM << 20),
        cost_estimate=pl.CostEstimate(flops=flops, transcendentals=0, bytes_accessed=1 << 20),
    )


def each_pair(pairs, work):
    def step(n, _):
        for i in range(STEP):
            work(n * STEP + i)
        return _

    lax.fori_loop(0, pairs // STEP, step, 0)


def relay_kernel(x_ref, o_ref, flat_ref, left_ref, right_ref):
    low = lax.broadcasted_iota(jnp.int32, (R // 2, 128), 1) < 64

    def work(g, _):
        rows = pl.ds(pl.multiple_of(g * 8, 8), 8)
        for j in range(CHUNKS):
            flat_ref[j * 8 : j * 8 + 8] = x_ref[rows, j * 128 : j * 128 + 128].astype(F32)
        for i in range(8):
            first, second, third = (
                flat_ref[pl.ds(n * 8 + i, R // 2, stride=24), :] for n in range(3)
            )
            second_turned, third_turned = pltpu.roll(second, 64, 1), pltpu.roll(third, 64, 1)
            left_ref[i, pl.ds(0, R // 2, stride=2), :] = first
            right_ref[i, pl.ds(0, R // 2, stride=2), :] = second
            left_ref[i, pl.ds(1, R // 2, stride=2), :] = jnp.where(low, second_turned, third_turned)
            right_ref[i, pl.ds(1, R // 2, stride=2), :] = third_turned
            o_ref[g * 8 + i, :, :128] = left_ref[i].astype(BF16)
            o_ref[g * 8 + i, :, 128:] = right_ref[i][:, :64].astype(BF16)
        return _

    lax.fori_loop(0, x_ref.shape[0] // 8, work, 0)


def relay(x):
    pairs = x.shape[0]
    return call(
        relay_kernel,
        [VMEM],
        jax.ShapeDtypeStruct((pairs, R, R), BF16),
        VMEM,
        [
            pltpu.VMEM((CHUNKS * 8, 128), F32),
            pltpu.VMEM((8, R, 128), F32),
            pltpu.VMEM((8, R, 128), F32),
        ],
        1 << 24,
    )(x)


def pack_kernel(x_ref, o_ref, flat_ref, left_ref, right_ref):
    low = lax.broadcasted_iota(jnp.int32, (R // 2, 128), 1) < 64
    for j in range(CHUNKS):
        flat_ref[j : j + 1] = x_ref[:, j * 128 : j * 128 + 128].astype(F32)
    first, second, third = (flat_ref[pl.ds(n, R // 2, stride=3), :] for n in range(3))
    second_turned, third_turned = pltpu.roll(second, 64, 1), pltpu.roll(third, 64, 1)
    left_ref[pl.ds(0, R // 2, stride=2), :] = first
    right_ref[pl.ds(0, R // 2, stride=2), :] = second
    left_ref[pl.ds(1, R // 2, stride=2), :] = jnp.where(low, second_turned, third_turned)
    right_ref[pl.ds(1, R // 2, stride=2), :] = third_turned
    block = jnp.concatenate([left_ref[...], right_ref[:, :64]], axis=1)
    for q in range(4):
        o_ref[q] = packed_quarter(block, q).astype(BF16)


def pack(x):
    return call(
        pack_kernel,
        [VMEM],
        jax.ShapeDtypeStruct((4, QP, 128), BF16),
        VMEM,
        [pltpu.VMEM((CHUNKS, 128), F32), pltpu.VMEM((R, 128), F32), pltpu.VMEM((R, 128), F32)],
        1 << 33,
    )(x)


def choose_kernel(at_ref, *refs):
    for n in range(4):
        refs[4][n] = refs[n][at_ref[3]]


def choose(at, near):
    return call(
        choose_kernel,
        [SMEM] + [VMEM] * 4,
        jax.ShapeDtypeStruct((4, QP, 128), BF16),
        VMEM,
        [],
        1 << 20,
    )(at, *near)


def lay_out(block, i, flat_ref, left_ref, right_ref):
    low = lax.broadcasted_iota(jnp.int32, (R // 2, 128), 1) < 64
    left_ref[i] = block[:, :128]
    right_ref[i, :, :64] = block[:, 128:]
    even = pl.ds(0, R // 2, stride=2)
    odd = pl.ds(1, R // 2, stride=2)
    turned = pltpu.roll(left_ref[i, odd, :], 64, 1)
    flat_ref[pl.ds(i, R // 2, stride=24), :] = left_ref[i, even, :]
    flat_ref[pl.ds(8 + i, R // 2, stride=24), :] = jnp.where(low, right_ref[i, even, :], turned)
    flat_ref[pl.ds(16 + i, R // 2, stride=24), :] = jnp.where(
        low, turned, pltpu.roll(right_ref[i, odd, :], 64, 1)
    )


def project_kernel(ends_ref, rank_ref, at_ref, s_ref, m_ref, p_ref, *rest):
    out_refs, sums_ref = rest[:8], rest[8]
    sums_ref[...] = jnp.zeros_like(sums_ref)

    def work(pair):
        inside = masks((rank_ref[pair] + 1) * RSTEP)
        masked = jnp.where(inside, m_ref[pair].astype(F32), 0.0).astype(BF16)
        half = dot(s_ref[pair], masked, ((1,), (0,))).astype(BF16)
        full = dot(half, s_ref[pair], ((1,), (1,)))
        p_ref[pair] = full.astype(BF16)
        for q in range(4):
            piece = packed_quarter(full, q).astype(BF16)
            for e in range(2):
                slot = slot_of(ends_ref[e, pair], q, at_ref)
                sums_ref[slot] = sums_ref[slot] + piece

    each_pair(s_ref.shape[0], work)
    for n in range(8):
        out_refs[n][...] = sums_ref[n * 32 : (n + 1) * 32].reshape(GROUP)


def project(ends, rank, at, s, m):
    pairs = s.shape[0]
    return call(
        project_kernel,
        [SMEM] * 3 + [VMEM] * 2,
        [jax.ShapeDtypeStruct((pairs, R, R), BF16)] + [jax.ShapeDtypeStruct(GROUP, BF16)] * 8,
        [VMEM] * 9,
        [pltpu.VMEM((256, QP, 128), BF16)],
        pairs * 4 * R**3,
    )(ends, rank, at, s, m)


def base_kernel(rank_ref, m_ref, v_ref, base_ref):
    def work(pair):
        inside = masks((rank_ref[pair] + 1) * RSTEP)
        masked = jnp.where(inside, m_ref[pair].astype(F32), 0.0).astype(BF16)
        base_ref[pair] = v_ref[pair].astype(F32) + dot(masked, v_ref[pair], ((1,), (0,)))

    each_pair(m_ref.shape[0], work)


def base_of(rank, m, v):
    pairs = m.shape[0]
    return call(
        base_kernel,
        [SMEM, VMEM, VMEM],
        jax.ShapeDtypeStruct((pairs, R, R), F32),
        VMEM,
        [],
        pairs * 2 * R**3,
    )(rank, m, v)


def own_kernel(ends_ref, at_ref, p_ref, *rest):
    group_refs, own_ref, held_ref = rest[:8], rest[8], rest[9]
    for n in range(8):
        held_ref[n * 32 : (n + 1) * 32] = group_refs[n][...].reshape(32, QP, 128)

    def work(pair):
        quarters = []
        for q in range(4):
            first = held_ref[slot_of(ends_ref[0, pair], q, at_ref)].astype(F32)
            second = held_ref[slot_of(ends_ref[1, pair], q, at_ref)].astype(F32)
            quarters.append(unpacked_quarter(first + second))
        both = jnp.concatenate(quarters, axis=0).astype(BF16)
        own = dot(p_ref[pair], both, ((1,), (0,)))
        for q in range(4):
            own_ref[pair, q] = packed_quarter(own, q).astype(BF16)

    each_pair(p_ref.shape[0], work)


def own_of(ends, at, p, groups):
    pairs = p.shape[0]
    return call(
        own_kernel,
        [SMEM] * 2 + [VMEM] * 9,
        jax.ShapeDtypeStruct((pairs, 4, QP, 128), BF16),
        VMEM,
        [pltpu.VMEM((256, QP, 128), BF16)],
        pairs * 2 * R**3,
    )(ends, at, p, *groups)


def couple_kernel(d0_ref, d1_ref, d2_ref, d3_ref, x0_ref, x1_ref, x2_ref, x3_ref, c_ref):
    for t, x_ref in enumerate((x0_ref, x1_ref, x2_ref, x3_ref)):
        total = d0_ref[t].astype(F32) + d1_ref[t ^ 1].astype(F32)
        total = total + (d2_ref[t ^ 2].astype(F32) + d3_ref[t ^ 3].astype(F32))
        domain = unpacked_quarter(total).astype(BF16)
        block = [unpacked_quarter(x_ref[q].astype(F32)) for q in range(4)]
        block = jnp.concatenate(block, axis=0).astype(BF16)
        c_ref[t] = packed_quarter(dot(domain, block, ((1,), (0,))), 0).astype(BF16)


def couple(parts, near):
    return call(
        couple_kernel, [VMEM] * 8, jax.ShapeDtypeStruct((4, QP, 128), BF16), VMEM, [], 8 * Q * R * R
    )(*parts, *near)


def finish_kernel(ends_ref, rank_ref, at_ref, s_ref, own_ref, base_ref, *rest):
    group_refs, out_ref, held_ref = rest[:8], rest[8], rest[9]
    flat_ref, left_ref, right_ref, rows_ref, sem = rest[10:]
    groups = s_ref.shape[0] // 8
    for n in range(8):
        held_ref[n * 32 : (n + 1) * 32] = group_refs[n][...].reshape(32, QP, 128)
    right_ref[...] = jnp.zeros_like(right_ref)

    def send(g):
        rows = pl.ds(pl.multiple_of(g * 8, 8), 8)
        return pltpu.make_async_copy(rows_ref.at[g], out_ref.at[rows], sem.at[g])

    def work(g, _):
        for i in range(8):
            pair = g * 8 + i
            quarters = []
            for q in range(4):
                first = held_ref[slot_of(ends_ref[0, pair], q, at_ref)].astype(F32)
                second = held_ref[slot_of(ends_ref[1, pair], q, at_ref)].astype(F32)
                quarters.append(unpacked_quarter((first + second) - own_ref[pair, q].astype(F32)))
            combined = jnp.concatenate(quarters, axis=0).astype(BF16)
            half = dot(s_ref[pair], combined, ((0,), (0,))).astype(BF16)
            total = base_ref[pair] + dot(half, s_ref[pair], ((1,), (0,)))
            inside = masks((rank_ref[pair] + 1) * RSTEP)
            lay_out(jnp.where(inside, total, 0.0), i, flat_ref, left_ref, right_ref)
        for j in range(CHUNKS):
            rows_ref[g, :, j * 128 : j * 128 + 128] = flat_ref[j * 8 : j * 8 + 8].astype(BF16)
        send(g).start()
        return _

    lax.fori_loop(0, groups, work, 0)
    for g in range(groups):
        send(g).wait()


def finish(ends, rank, at, s, own, base, groups):
    pairs = s.shape[0]
    return call(
        finish_kernel,
        [SMEM] * 3 + [VMEM] * 11,
        jax.ShapeDtypeStruct((pairs, R * R), BF16),
        HBM,
        [
            pltpu.VMEM((256, QP, 128), BF16),
            pltpu.VMEM((CHUNKS * 8, 128), F32),
            pltpu.VMEM((8, R, 128), F32),
            pltpu.VMEM((8, R, 128), F32),
            pltpu.VMEM((pairs // 8, 8, R * R), BF16),
            pltpu.SemaphoreType.DMA((pairs // 8,)),
        ],
        pairs * 4 * R**3,
    )(ends, rank, at, s, own, base, *groups)


def added(*arrays):
    total = arrays[0].astype(F32)
    for a in arrays[1:]:
        total = total + a.astype(F32)
    return total.astype(BF16)


def sent_to_all(mine):
    both = jnp.concatenate([mine, stage_z(mine, 1)], axis=0)
    group = [both] + [stage_b(both, d) for d in (1, 2, 3)]
    group = jnp.stack(group, axis=0)
    groups = [group] + [stage_a(group, d) for d in (2, 1, 3)]
    groups = [groups[0], groups[2], groups[1], groups[3]]
    return groups + [stage_c(groups[n]) for n in range(4)]


def whole_step(pair_list, rank_bucket, amplitudes, intersects, integrals, exchange_blocks):
    at = jnp.stack([lax.axis_index(a) for a in AXES]).astype(jnp.int32)
    ends = pair_list.T

    block = pack(exchange_blocks)
    pair = jnp.stack([block, stage_z(block, 2)])
    far = stage_z(pair, 6)
    near = [pair[0], pair[1], far[1], far[0]]
    quarters = choose(at, near)
    blocks = sent_to_all(quarters)

    m = relay(amplitudes)
    s = relay(intersects)
    p, *sums = project(ends, rank_bucket, at, s, m)
    v = relay(integrals)
    base = base_of(rank_bucket, m, v)

    sums = [added(sums[a], stage_c(sums[4 + a])) for a in (2, 1, 3, 0)]
    moved = [stage_a(sums[n], d) for n, d in enumerate((2, 1, 3))]
    sums = added(sums[3], *moved)
    sums = added(sums[0], *[stage_b(sums[d], d) for d in (1, 2, 3)])
    sums = added(sums[:4], stage_z(sums[4:], 1))
    parts = [sums] + [stage_z(sums, 2 * d) for d in (1, 2, 3)]
    coupled = couple(parts, near)
    own = own_of(ends, at, p, blocks)
    groups = sent_to_all(coupled)
    return finish(ends, rank_bucket, at, s, own, base, groups)


def solution(mesh):
    torus = Mesh(mesh.devices.reshape(4, 2, mesh.shape["gy"], mesh.shape["gz"]), AXES)
    everywhere = P(AXES, None)
    return jax.shard_map(
        whole_step,
        mesh=torus,
        in_specs=(everywhere, P(AXES), everywhere, everywhere, everywhere, P(GX_GY, None)),
        out_specs=everywhere,
        check_vma=False,
    )
```

```python
import jax
import jax.numpy as jnp
from jax import lax
from jax.experimental import pallas as pl
from jax.experimental.pallas import tpu as pltpu
from jax.sharding import Mesh
from jax.sharding import PartitionSpec as P

RSTEP = 64
R = 192
Q = 48
QP = 72
CHUNKS = R * R // 128
EVEN = (0, 3, 5, 6)
STEP = 8
AXES = ("gx_0", "gx_1", "gy", "gz")
GX_GY = ("gx_0", "gx_1", "gy")
BF16 = jnp.bfloat16
F32 = jnp.float32


def device_number(x, c, z, y):
    return ((x * 2 + c) * 8 + z) * 4 + y


def pairs_of(move):
    out = []
    for x in range(4):
        for c in range(2):
            for z in range(8):
                for y in range(4):
                    out.append((device_number(x, c, z, y), device_number(*move(x, c, z, y))))
    return out


def stage_a(array, d):
    return lax.ppermute(
        array, AXES, pairs_of(lambda x, c, z, y: (x ^ d, c, z, y) if c == 0 else (x, c, z, y ^ d))
    )


def stage_b(array, d):
    return lax.ppermute(
        array, AXES, pairs_of(lambda x, c, z, y: (x, c, z, y ^ d) if c == 0 else (x ^ d, c, z, y))
    )


def stage_z(array, d):
    return lax.ppermute(array, AXES, pairs_of(lambda x, c, z, y: (x, c, z ^ d, y)))


def stage_c(array):
    return lax.ppermute(array, AXES, pairs_of(lambda x, c, z, y: (x, c ^ 1, z, y)))


def slot_of(k, q, at_ref):
    x, c, z, y = (at_ref[i] for i in range(4))
    core = (k >> 3) & 1
    dx, dq, dz = (k >> 4) ^ x, q ^ y, (k & 7) ^ z
    a = jnp.where(core == 0, dx, dq)
    b = jnp.where(core == 0, dq, dx)
    odd = (dz ^ (dz >> 1) ^ (dz >> 2)) & 1
    return (((core ^ c) * 4 + a) * 4 + b) * 8 + odd * 4 + (dz >> 1)


def packed_quarter(block, q):
    rows = block[q * Q : (q + 1) * Q]
    right = jnp.concatenate([rows[: Q // 2, 128:], rows[Q // 2 :, 128:]], axis=1)
    return jnp.concatenate([rows[:, :128], right], axis=0)


def unpacked_quarter(piece):
    right = piece[Q:]
    right = jnp.concatenate([right[:, :64], right[:, 64:]], axis=0)
    return jnp.concatenate([piece[:Q], right], axis=1)


def masks(rank):
    rows = lax.broadcasted_iota(jnp.int32, (R, R), 0)
    cols = lax.broadcasted_iota(jnp.int32, (R, R), 1)
    return (rows < rank) & (cols < rank)


def dot(a, b, dims):
    return lax.dot_general(a, b, (dims, ((), ())), preferred_element_type=F32)


VLIM = 14

SMEM = pl.BlockSpec(memory_space=pltpu.SMEM)
VMEM = pl.BlockSpec(memory_space=pltpu.VMEM)
HBM = pl.BlockSpec(memory_space=pltpu.HBM)
ANY = pl.BlockSpec(memory_space=pl.ANY)
GROUP = (4, 8, QP, 128)


def call(kernel, in_specs, out_shape, out_specs, scratch, flops):
    return pl.pallas_call(
        kernel,
        in_specs=in_specs,
        out_specs=out_specs,
        out_shape=out_shape,
        scratch_shapes=scratch,
        compiler_params=pltpu.CompilerParams(vmem_limit_bytes=VLIM << 20),
        cost_estimate=pl.CostEstimate(flops=flops, transcendentals=0, bytes_accessed=1 << 20),
    )


def each_pair(pairs, work):
    def step(n, _):
        for i in range(STEP):
            work(n * STEP + i)
        return _

    lax.fori_loop(0, pairs // STEP, step, 0)


def relay_kernel(x_ref, o_ref, flat_ref, left_ref, right_ref):
    low = lax.broadcasted_iota(jnp.int32, (R // 2, 128), 1) < 64

    def work(g, _):
        rows = pl.ds(pl.multiple_of(g * 8, 8), 8)
        for j in range(CHUNKS):
            flat_ref[j * 8 : j * 8 + 8] = x_ref[rows, j * 128 : j * 128 + 128].astype(F32)
        for i in range(8):
            first, second, third = (
                flat_ref[pl.ds(n * 8 + i, R // 2, stride=24), :] for n in range(3)
            )
            second_turned, third_turned = pltpu.roll(second, 64, 1), pltpu.roll(third, 64, 1)
            left_ref[i, pl.ds(0, R // 2, stride=2), :] = first
            right_ref[i, pl.ds(0, R // 2, stride=2), :] = second
            left_ref[i, pl.ds(1, R // 2, stride=2), :] = jnp.where(low, second_turned, third_turned)
            right_ref[i, pl.ds(1, R // 2, stride=2), :] = third_turned
            o_ref[g * 8 + i, :, :128] = left_ref[i].astype(BF16)
            o_ref[g * 8 + i, :, 128:] = right_ref[i][:, :64].astype(BF16)
        return _

    lax.fori_loop(0, x_ref.shape[0] // 8, work, 0)


def relay(x):
    pairs = x.shape[0]
    return call(
        relay_kernel,
        [VMEM],
        jax.ShapeDtypeStruct((pairs, R, R), BF16),
        VMEM,
        [
            pltpu.VMEM((CHUNKS * 8, 128), F32),
            pltpu.VMEM((8, R, 128), F32),
            pltpu.VMEM((8, R, 128), F32),
        ],
        1 << 24,
    )(x)


def pack_kernel(x_ref, o_ref, flat_ref, left_ref, right_ref):
    low = lax.broadcasted_iota(jnp.int32, (R // 2, 128), 1) < 64
    for j in range(CHUNKS):
        flat_ref[j : j + 1] = x_ref[:, j * 128 : j * 128 + 128].astype(F32)
    first, second, third = (flat_ref[pl.ds(n, R // 2, stride=3), :] for n in range(3))
    second_turned, third_turned = pltpu.roll(second, 64, 1), pltpu.roll(third, 64, 1)
    left_ref[pl.ds(0, R // 2, stride=2), :] = first
    right_ref[pl.ds(0, R // 2, stride=2), :] = second
    left_ref[pl.ds(1, R // 2, stride=2), :] = jnp.where(low, second_turned, third_turned)
    right_ref[pl.ds(1, R // 2, stride=2), :] = third_turned
    block = jnp.concatenate([left_ref[...], right_ref[:, :64]], axis=1)
    for q in range(4):
        o_ref[q] = packed_quarter(block, q).astype(BF16)


def pack(x):
    return call(
        pack_kernel,
        [VMEM],
        jax.ShapeDtypeStruct((4, QP, 128), BF16),
        VMEM,
        [pltpu.VMEM((CHUNKS, 128), F32), pltpu.VMEM((R, 128), F32), pltpu.VMEM((R, 128), F32)],
        1 << 33,
    )(x)


def choose_kernel(at_ref, *refs):
    for n in range(4):
        refs[4][n] = refs[n][at_ref[3]]


def choose(at, near):
    return call(
        choose_kernel,
        [SMEM] + [VMEM] * 4,
        jax.ShapeDtypeStruct((4, QP, 128), BF16),
        VMEM,
        [],
        1 << 20,
    )(at, *near)


def copy_kernel(x_ref, o_ref):
    o_ref[...] = x_ref[...]


def copied(x):
    return call(copy_kernel, [VMEM], jax.ShapeDtypeStruct(x.shape, x.dtype), VMEM, [], 1)(x)


def lay_out(block, i, flat_ref, left_ref, right_ref):
    low = lax.broadcasted_iota(jnp.int32, (R // 2, 128), 1) < 64
    left_ref[i] = block[:, :128]
    right_ref[i, :, :64] = block[:, 128:]
    even = pl.ds(0, R // 2, stride=2)
    odd = pl.ds(1, R // 2, stride=2)
    turned = pltpu.roll(left_ref[i, odd, :], 64, 1)
    flat_ref[pl.ds(i, R // 2, stride=24), :] = left_ref[i, even, :]
    flat_ref[pl.ds(8 + i, R // 2, stride=24), :] = jnp.where(low, right_ref[i, even, :], turned)
    flat_ref[pl.ds(16 + i, R // 2, stride=24), :] = jnp.where(
        low, turned, pltpu.roll(right_ref[i, odd, :], 64, 1)
    )


def project_kernel(ends_in, rank_in, at_in, s_ref, m_ref, p_ref, *rest):
    out_refs, sums_ref, ends_ref, rank_ref, at_ref, sem = rest[:8], *rest[8:]
    copies = [
        pltpu.make_async_copy(a, b, sem.at[n])
        for n, (a, b) in enumerate(((ends_in, ends_ref), (rank_in, rank_ref), (at_in, at_ref)))
    ]
    for copy in copies:
        copy.start()
    sums_ref[...] = jnp.zeros_like(sums_ref)
    for copy in copies:
        copy.wait()

    def work(pair):
        inside = masks((rank_ref[pair] + 1) * RSTEP)
        masked = jnp.where(inside, m_ref[pair].astype(F32), 0.0).astype(BF16)
        half = dot(s_ref[pair], masked, ((1,), (0,))).astype(BF16)
        full = dot(half, s_ref[pair], ((1,), (1,)))
        p_ref[pair] = full.astype(BF16)
        for q in range(4):
            piece = packed_quarter(full, q).astype(BF16)
            for e in range(2):
                slot = slot_of(ends_ref[e, pair], q, at_ref)
                sums_ref[slot] = sums_ref[slot] + piece

    each_pair(s_ref.shape[0], work)
    for n in range(8):
        out_refs[n][...] = sums_ref[n * 32 : (n + 1) * 32].reshape(GROUP)


def project(ends, rank, at, s, m):
    pairs = s.shape[0]
    return call(
        project_kernel,
        [ANY] * 3 + [VMEM] * 2,
        [jax.ShapeDtypeStruct((pairs, R, R), BF16)] + [jax.ShapeDtypeStruct(GROUP, BF16)] * 8,
        [VMEM] * 9,
        [pltpu.VMEM((256, QP, 128), BF16)]
        + [pltpu.SMEM(f.shape, jnp.int32) for f in (ends, rank, at)]
        + [pltpu.SemaphoreType.DMA((3,))],
        pairs * 4 * R**3,
    )(ends, rank, at, s, m)


def base_kernel(rank_ref, m_ref, v_ref, base_ref):
    def work(pair):
        inside = masks((rank_ref[pair] + 1) * RSTEP)
        masked = jnp.where(inside, m_ref[pair].astype(F32), 0.0).astype(BF16)
        base_ref[pair] = v_ref[pair].astype(F32) + dot(masked, v_ref[pair], ((1,), (0,)))

    each_pair(m_ref.shape[0], work)


def base_of(rank, m, v):
    pairs = m.shape[0]
    return call(
        base_kernel,
        [SMEM, VMEM, VMEM],
        jax.ShapeDtypeStruct((pairs, R, R), F32),
        VMEM,
        [],
        pairs * 2 * R**3,
    )(rank, m, v)


def own_kernel(ends_ref, at_ref, p_ref, *rest):
    group_refs, own_ref, held_ref = rest[:8], rest[8], rest[9]
    for n in range(8):
        held_ref[n * 32 : (n + 1) * 32] = group_refs[n][...].reshape(32, QP, 128)

    def work(pair):
        quarters = []
        for q in range(4):
            first = held_ref[slot_of(ends_ref[0, pair], q, at_ref)].astype(F32)
            second = held_ref[slot_of(ends_ref[1, pair], q, at_ref)].astype(F32)
            quarters.append(unpacked_quarter(first + second))
        both = jnp.concatenate(quarters, axis=0).astype(BF16)
        own = dot(p_ref[pair], both, ((1,), (0,)))
        for q in range(4):
            own_ref[pair, q] = packed_quarter(own, q).astype(BF16)

    each_pair(p_ref.shape[0], work)


def own_of(ends, at, p, groups):
    pairs = p.shape[0]
    return call(
        own_kernel,
        [SMEM] * 2 + [VMEM] * 9,
        jax.ShapeDtypeStruct((pairs, 4, QP, 128), BF16),
        VMEM,
        [pltpu.VMEM((256, QP, 128), BF16)],
        pairs * 2 * R**3,
    )(ends, at, p, *groups)


def couple_kernel(d0_ref, d1_ref, d2_ref, d3_ref, x0_ref, x1_ref, x2_ref, x3_ref, c_ref):
    for t, x_ref in enumerate((x0_ref, x1_ref, x2_ref, x3_ref)):
        total = d0_ref[t].astype(F32) + d1_ref[t ^ 1].astype(F32)
        total = total + (d2_ref[t ^ 2].astype(F32) + d3_ref[t ^ 3].astype(F32))
        domain = unpacked_quarter(total).astype(BF16)
        block = [unpacked_quarter(x_ref[q].astype(F32)) for q in range(4)]
        block = jnp.concatenate(block, axis=0).astype(BF16)
        c_ref[t] = packed_quarter(dot(domain, block, ((1,), (0,))), 0).astype(BF16)


def couple(parts, near):
    return call(
        couple_kernel, [VMEM] * 8, jax.ShapeDtypeStruct((4, QP, 128), BF16), VMEM, [], 8 * Q * R * R
    )(*parts, *near)


def finish_kernel(ends_in, rank_in, at_in, s_ref, own_ref, base_ref, *rest):
    group_refs, out_ref, held_ref = rest[:8], rest[8], rest[9]
    flat_ref, left_ref, right_ref, rows_ref, sem, ends_ref, rank_ref, at_ref, facts_sem = rest[10:]
    groups = s_ref.shape[0] // 8
    copies = [
        pltpu.make_async_copy(a, b, facts_sem.at[n])
        for n, (a, b) in enumerate(((ends_in, ends_ref), (rank_in, rank_ref), (at_in, at_ref)))
    ]
    for copy in copies:
        copy.start()
    for n in range(8):
        held_ref[n * 32 : (n + 1) * 32] = group_refs[n][...].reshape(32, QP, 128)
    right_ref[...] = jnp.zeros_like(right_ref)
    for copy in copies:
        copy.wait()

    def send(g):
        rows = pl.ds(pl.multiple_of(g * 8, 8), 8)
        return pltpu.make_async_copy(rows_ref.at[g], out_ref.at[rows], sem.at[g])

    def work(g, _):
        for i in range(8):
            pair = g * 8 + i
            quarters = []
            for q in range(4):
                first = held_ref[slot_of(ends_ref[0, pair], q, at_ref)].astype(F32)
                second = held_ref[slot_of(ends_ref[1, pair], q, at_ref)].astype(F32)
                quarters.append(unpacked_quarter((first + second) - own_ref[pair, q].astype(F32)))
            combined = jnp.concatenate(quarters, axis=0).astype(BF16)
            half = dot(s_ref[pair], combined, ((0,), (0,))).astype(BF16)
            total = base_ref[pair] + dot(half, s_ref[pair], ((1,), (0,)))
            inside = masks((rank_ref[pair] + 1) * RSTEP)
            lay_out(jnp.where(inside, total, 0.0), i, flat_ref, left_ref, right_ref)
        for j in range(CHUNKS):
            rows_ref[g, :, j * 128 : j * 128 + 128] = flat_ref[j * 8 : j * 8 + 8].astype(BF16)
        send(g).start()
        return _

    lax.fori_loop(0, groups, work, 0)
    for g in range(groups):
        send(g).wait()


def finish(ends, rank, at, s, own, base, groups):
    pairs = s.shape[0]
    return call(
        finish_kernel,
        [ANY] * 3 + [VMEM] * 11,
        jax.ShapeDtypeStruct((pairs, R * R), BF16),
        HBM,
        [
            pltpu.VMEM((256, QP, 128), BF16),
            pltpu.VMEM((CHUNKS * 8, 128), F32),
            pltpu.VMEM((8, R, 128), F32),
            pltpu.VMEM((8, R, 128), F32),
            pltpu.VMEM((pairs // 8, 8, R * R), BF16),
            pltpu.SemaphoreType.DMA((pairs // 8,)),
            pltpu.SMEM(ends.shape, jnp.int32),
            pltpu.SMEM(rank.shape, jnp.int32),
            pltpu.SMEM(at.shape, jnp.int32),
            pltpu.SemaphoreType.DMA((3,)),
        ],
        pairs * 4 * R**3,
    )(ends, rank, at, s, own, base, *groups)


def added(*arrays):
    total = arrays[0].astype(F32)
    for a in arrays[1:]:
        total = total + a.astype(F32)
    return total.astype(BF16)


def sent_to_all(mine):
    both = jnp.concatenate([mine, stage_z(mine, 1)], axis=0)
    group = [both] + [stage_b(both, d) for d in (1, 2, 3)]
    group = jnp.stack(group, axis=0)
    groups = [group] + [stage_a(group, d) for d in (2, 1, 3)]
    groups = [groups[0], groups[2], groups[1], groups[3]]
    return groups + [stage_c(groups[n]) for n in range(4)]


def whole_step(pair_list, rank_bucket, amplitudes, intersects, integrals, exchange_blocks):
    at = jnp.stack([lax.axis_index(a) for a in AXES]).astype(jnp.int32)
    ends = pair_list.T

    block = pack(exchange_blocks)
    pair = jnp.stack([block, stage_z(block, EVEN[1])])
    far = stage_z(pair, EVEN[3])
    near = [pair[0], pair[1], far[1], far[0]]
    quarters = choose(at, near)
    blocks = sent_to_all(quarters)

    m = relay(amplitudes)
    s = relay(intersects)
    p, *sums = project(ends, rank_bucket, at, s, m)
    v = relay(integrals)
    base = base_of(rank_bucket, m, v)

    sums = [added(sums[a], stage_c(sums[4 + a])) for a in (1, 3, 2, 0)]
    moved = [stage_a(sums[n], d) for n, d in enumerate((1, 3, 2))]
    sums = added(sums[3], *moved)
    sums = added(sums[0], *[stage_b(sums[d], d) for d in (1, 2, 3)])
    sums = added(sums[:4], stage_z(sums[4:], 1))
    parts = [sums] + [stage_z(sums, EVEN[d]) for d in (1, 2, 3)]
    near[0] = copied(near[0])
    coupled = couple(parts, near)
    own = own_of(ends, at, p, blocks)
    groups = sent_to_all(coupled)
    return finish(ends, rank_bucket, at, s, own, base, groups)


def solution(mesh):
    torus = Mesh(mesh.devices.reshape(4, 2, mesh.shape["gy"], mesh.shape["gz"]), AXES)
    everywhere = P(AXES, None)
    return jax.shard_map(
        whole_step,
        mesh=torus,
        in_specs=(everywhere, P(AXES), everywhere, everywhere, everywhere, P(GX_GY, None)),
        out_specs=everywhere,
        check_vma=False,
    )
```

```python
import functools
import jax
import jax.numpy as jnp
from jax import lax
from jax.experimental import pallas as pl
from jax.experimental.pallas import tpu as pltpu
from jax.sharding import Mesh
from jax.sharding import PartitionSpec as P

RSTEP = 64
R = 192
Q = 48
QP = 72
CHUNKS = R * R // 128
EVEN = (0, 3, 5, 6)
STEP = 8
AXES = ("gx_0", "gx_1", "gy", "gz")
GX_GY = ("gx_0", "gx_1", "gy")
BF16 = jnp.bfloat16
F32 = jnp.float32


def device_number(x, c, z, y):
    return ((x * 2 + c) * 8 + z) * 4 + y


def pairs_of(move):
    out = []
    for x in range(4):
        for c in range(2):
            for z in range(8):
                for y in range(4):
                    out.append((device_number(x, c, z, y), device_number(*move(x, c, z, y))))
    return out


def stage_a(array, d):
    return lax.ppermute(
        array, AXES, pairs_of(lambda x, c, z, y: (x ^ d, c, z, y) if c == 0 else (x, c, z, y ^ d))
    )


def stage_b(array, d):
    return lax.ppermute(
        array, AXES, pairs_of(lambda x, c, z, y: (x, c, z, y ^ d) if c == 0 else (x ^ d, c, z, y))
    )


def stage_z(array, d):
    return lax.ppermute(array, AXES, pairs_of(lambda x, c, z, y: (x, c, z ^ d, y)))


def stage_c(array):
    return lax.ppermute(array, AXES, pairs_of(lambda x, c, z, y: (x, c ^ 1, z, y)))


def slot_of(k, q, at_ref):
    x, c, z, y = (at_ref[i] for i in range(4))
    core = (k >> 3) & 1
    dx, dq, dz = (k >> 4) ^ x, q ^ y, (k & 7) ^ z
    a = jnp.where(core == 0, dx, dq)
    b = jnp.where(core == 0, dq, dx)
    odd = (dz ^ (dz >> 1) ^ (dz >> 2)) & 1
    return (((core ^ c) * 4 + a) * 4 + b) * 8 + odd * 4 + (dz >> 1)


def packed_quarter(block, q):
    rows = block[q * Q : (q + 1) * Q]
    right = jnp.concatenate([rows[: Q // 2, 128:], rows[Q // 2 :, 128:]], axis=1)
    return jnp.concatenate([rows[:, :128], right], axis=0)


def unpacked_quarter(piece):
    right = piece[Q:]
    right = jnp.concatenate([right[:, :64], right[:, 64:]], axis=0)
    return jnp.concatenate([piece[:Q], right], axis=1)


def masks(rank):
    rows = lax.broadcasted_iota(jnp.int32, (R, R), 0)
    cols = lax.broadcasted_iota(jnp.int32, (R, R), 1)
    return (rows < rank) & (cols < rank)


def dot(a, b, dims):
    return lax.dot_general(a, b, (dims, ((), ())), preferred_element_type=F32)


VLIM = 14

SMEM = pl.BlockSpec(memory_space=pltpu.SMEM)
VMEM = pl.BlockSpec(memory_space=pltpu.VMEM)
HBM = pl.BlockSpec(memory_space=pltpu.HBM)
ANY = pl.BlockSpec(memory_space=pl.ANY)
GROUP = (4, 8, QP, 128)


def call(kernel, in_specs, out_shape, out_specs, scratch, flops):
    return pl.pallas_call(
        kernel,
        in_specs=in_specs,
        out_specs=out_specs,
        out_shape=out_shape,
        scratch_shapes=scratch,
        compiler_params=pltpu.CompilerParams(vmem_limit_bytes=VLIM << 20),
        cost_estimate=pl.CostEstimate(flops=flops, transcendentals=0, bytes_accessed=1 << 20),
    )


def each_pair(pairs, work):
    def step(n, _):
        for i in range(STEP):
            work(n * STEP + i)
        return _

    lax.fori_loop(0, pairs // STEP, step, 0)


def relay_kernel(x_ref, o_ref, flat_ref, left_ref, right_ref):
    low = lax.broadcasted_iota(jnp.int32, (R // 2, 128), 1) < 64

    def work(g, _):
        rows = pl.ds(pl.multiple_of(g * 8, 8), 8)
        for j in range(CHUNKS):
            flat_ref[j * 8 : j * 8 + 8] = x_ref[rows, j * 128 : j * 128 + 128].astype(F32)
        for i in range(8):
            first, second, third = (
                flat_ref[pl.ds(n * 8 + i, R // 2, stride=24), :] for n in range(3)
            )
            second_turned, third_turned = pltpu.roll(second, 64, 1), pltpu.roll(third, 64, 1)
            left_ref[i, pl.ds(0, R // 2, stride=2), :] = first
            right_ref[i, pl.ds(0, R // 2, stride=2), :] = second
            left_ref[i, pl.ds(1, R // 2, stride=2), :] = jnp.where(low, second_turned, third_turned)
            right_ref[i, pl.ds(1, R // 2, stride=2), :] = third_turned
            o_ref[g * 8 + i, :, :128] = left_ref[i].astype(BF16)
            o_ref[g * 8 + i, :, 128:] = right_ref[i][:, :64].astype(BF16)
        return _

    lax.fori_loop(0, x_ref.shape[0] // 8, work, 0)


def relay(x):
    pairs = x.shape[0]
    return call(
        relay_kernel,
        [VMEM],
        jax.ShapeDtypeStruct((pairs, R, R), BF16),
        VMEM,
        [
            pltpu.VMEM((CHUNKS * 8, 128), F32),
            pltpu.VMEM((8, R, 128), F32),
            pltpu.VMEM((8, R, 128), F32),
        ],
        1 << 24,
    )(x)


def pack_kernel(x_ref, o_ref, flat_ref, left_ref, right_ref):
    low = lax.broadcasted_iota(jnp.int32, (R // 2, 128), 1) < 64
    for j in range(CHUNKS):
        flat_ref[j : j + 1] = x_ref[:, j * 128 : j * 128 + 128].astype(F32)
    first, second, third = (flat_ref[pl.ds(n, R // 2, stride=3), :] for n in range(3))
    second_turned, third_turned = pltpu.roll(second, 64, 1), pltpu.roll(third, 64, 1)
    left_ref[pl.ds(0, R // 2, stride=2), :] = first
    right_ref[pl.ds(0, R // 2, stride=2), :] = second
    left_ref[pl.ds(1, R // 2, stride=2), :] = jnp.where(low, second_turned, third_turned)
    right_ref[pl.ds(1, R // 2, stride=2), :] = third_turned
    block = jnp.concatenate([left_ref[...], right_ref[:, :64]], axis=1)
    for q in range(4):
        o_ref[q] = packed_quarter(block, q).astype(BF16)


def pack(x):
    return call(
        pack_kernel,
        [VMEM],
        jax.ShapeDtypeStruct((4, QP, 128), BF16),
        VMEM,
        [pltpu.VMEM((CHUNKS, 128), F32), pltpu.VMEM((R, 128), F32), pltpu.VMEM((R, 128), F32)],
        1 << 33,
    )(x)


def choose_kernel(at_ref, *refs):
    for n in range(4):
        refs[4][n] = refs[n][at_ref[3]]


def choose(at, near):
    return call(
        choose_kernel,
        [SMEM] + [VMEM] * 4,
        jax.ShapeDtypeStruct((4, QP, 128), BF16),
        VMEM,
        [],
        1 << 20,
    )(at, *near)


def copy_kernel(x_ref, o_ref):
    o_ref[...] = x_ref[...]


def copied(x):
    return call(copy_kernel, [VMEM], jax.ShapeDtypeStruct(x.shape, x.dtype), VMEM, [], 1)(x)


def lay_out(block, i, flat_ref, left_ref, right_ref):
    low = lax.broadcasted_iota(jnp.int32, (R // 2, 128), 1) < 64
    left_ref[i] = block[:, :128]
    right_ref[i, :, :64] = block[:, 128:]
    even = pl.ds(0, R // 2, stride=2)
    odd = pl.ds(1, R // 2, stride=2)
    turned = pltpu.roll(left_ref[i, odd, :], 64, 1)
    flat_ref[pl.ds(i, R // 2, stride=24), :] = left_ref[i, even, :]
    flat_ref[pl.ds(8 + i, R // 2, stride=24), :] = jnp.where(low, right_ref[i, even, :], turned)
    flat_ref[pl.ds(16 + i, R // 2, stride=24), :] = jnp.where(
        low, turned, pltpu.roll(right_ref[i, odd, :], 64, 1)
    )


def project_kernel(ends_in, rank_in, at_in, s_ref, m_ref, p_ref, *rest):
    out_refs, sums_ref, ends_ref, rank_ref, at_ref, sem = rest[:8], *rest[8:]
    copies = [
        pltpu.make_async_copy(a, b, sem.at[n])
        for n, (a, b) in enumerate(((ends_in, ends_ref), (rank_in, rank_ref), (at_in, at_ref)))
    ]
    for copy in copies:
        copy.start()
    sums_ref[...] = jnp.zeros_like(sums_ref)
    for copy in copies:
        copy.wait()

    def work(pair):
        inside = masks((rank_ref[pair] + 1) * RSTEP)
        masked = jnp.where(inside, m_ref[pair].astype(F32), 0.0).astype(BF16)
        half = dot(s_ref[pair], masked, ((1,), (0,))).astype(BF16)
        full = dot(half, s_ref[pair], ((1,), (1,)))
        p_ref[pair] = full.astype(BF16)
        for q in range(4):
            piece = packed_quarter(full, q).astype(BF16)
            for e in range(2):
                slot = slot_of(ends_ref[e, pair], q, at_ref)
                sums_ref[slot] = sums_ref[slot] + piece

    each_pair(s_ref.shape[0], work)
    for n in range(8):
        out_refs[n][...] = sums_ref[n * 32 : (n + 1) * 32].reshape(GROUP)


def project(ends, rank, at, s, m):
    pairs = s.shape[0]
    return call(
        project_kernel,
        [ANY] * 3 + [VMEM] * 2,
        [jax.ShapeDtypeStruct((pairs, R, R), BF16)] + [jax.ShapeDtypeStruct(GROUP, BF16)] * 8,
        [VMEM] * 9,
        [pltpu.VMEM((256, QP, 128), BF16)]
        + [pltpu.SMEM(f.shape, jnp.int32) for f in (ends, rank, at)]
        + [pltpu.SemaphoreType.DMA((3,))],
        pairs * 4 * R**3,
    )(ends, rank, at, s, m)


def base_kernel(rank_ref, m_ref, v_ref, base_ref):
    def work(pair):
        inside = masks((rank_ref[pair] + 1) * RSTEP)
        masked = jnp.where(inside, m_ref[pair].astype(F32), 0.0).astype(BF16)
        base_ref[pair] = v_ref[pair].astype(F32) + dot(masked, v_ref[pair], ((1,), (0,)))

    each_pair(m_ref.shape[0], work)


def base_of(rank, m, v):
    pairs = m.shape[0]
    return call(
        base_kernel,
        [SMEM, VMEM, VMEM],
        jax.ShapeDtypeStruct((pairs, R, R), F32),
        VMEM,
        [],
        pairs * 2 * R**3,
    )(rank, m, v)


def own_kernel(ends_ref, at_ref, p_ref, *rest):
    group_refs, own_ref, held_ref = rest[:8], rest[8], rest[9]
    for n in range(8):
        held_ref[n * 32 : (n + 1) * 32] = group_refs[n][...].reshape(32, QP, 128)

    def work(pair):
        quarters = []
        for q in range(4):
            first = held_ref[slot_of(ends_ref[0, pair], q, at_ref)].astype(F32)
            second = held_ref[slot_of(ends_ref[1, pair], q, at_ref)].astype(F32)
            quarters.append(unpacked_quarter(first + second))
        both = jnp.concatenate(quarters, axis=0).astype(BF16)
        own = dot(p_ref[pair], both, ((1,), (0,)))
        for q in range(4):
            own_ref[pair, q] = packed_quarter(own, q).astype(BF16)

    each_pair(p_ref.shape[0], work)


def own_of(ends, at, p, groups):
    pairs = p.shape[0]
    return call(
        own_kernel,
        [SMEM] * 2 + [VMEM] * 9,
        jax.ShapeDtypeStruct((pairs, 4, QP, 128), BF16),
        VMEM,
        [pltpu.VMEM((256, QP, 128), BF16)],
        pairs * 2 * R**3,
    )(ends, at, p, *groups)


def couple_kernel(d0_ref, d1_ref, d2_ref, d3_ref, x0_ref, x1_ref, x2_ref, x3_ref, c_ref):
    for t, x_ref in enumerate((x0_ref, x1_ref, x2_ref, x3_ref)):
        total = d0_ref[t].astype(F32) + d1_ref[t ^ 1].astype(F32)
        total = total + (d2_ref[t ^ 2].astype(F32) + d3_ref[t ^ 3].astype(F32))
        domain = unpacked_quarter(total).astype(BF16)
        block = [unpacked_quarter(x_ref[q].astype(F32)) for q in range(4)]
        block = jnp.concatenate(block, axis=0).astype(BF16)
        c_ref[t] = packed_quarter(dot(domain, block, ((1,), (0,))), 0).astype(BF16)


def couple(parts, near):
    return call(
        couple_kernel, [VMEM] * 8, jax.ShapeDtypeStruct((4, QP, 128), BF16), VMEM, [], 8 * Q * R * R
    )(*parts, *near)


def finish_kernel(ends_in, rank_in, at_in, s_ref, own_ref, base_ref, *rest, count):
    group_refs, rest = rest[:count], rest[count:]
    out_ref, held_ref = rest[:2]
    flat_ref, left_ref, right_ref, rows_ref, sem, ends_ref, rank_ref, at_ref, facts_sem = rest[2:]
    groups = s_ref.shape[0] // 8
    copies = [
        pltpu.make_async_copy(a, b, facts_sem.at[n])
        for n, (a, b) in enumerate(((ends_in, ends_ref), (rank_in, rank_ref), (at_in, at_ref)))
    ]
    for copy in copies:
        copy.start()
    at_slot = 0
    for ref in group_refs:
        slots = ref.shape[0] * ref.shape[1]
        held_ref[at_slot : at_slot + slots] = ref[...].reshape(slots, QP, 128)
        at_slot += slots
    right_ref[...] = jnp.zeros_like(right_ref)
    for copy in copies:
        copy.wait()

    def send(g):
        rows = pl.ds(pl.multiple_of(g * 8, 8), 8)
        return pltpu.make_async_copy(rows_ref.at[g], out_ref.at[rows], sem.at[g])

    def work(g, _):
        for i in range(8):
            pair = g * 8 + i
            quarters = []
            for q in range(4):
                first = held_ref[slot_of(ends_ref[0, pair], q, at_ref)].astype(F32)
                second = held_ref[slot_of(ends_ref[1, pair], q, at_ref)].astype(F32)
                quarters.append(unpacked_quarter((first + second) - own_ref[pair, q].astype(F32)))
            combined = jnp.concatenate(quarters, axis=0).astype(BF16)
            half = dot(s_ref[pair], combined, ((0,), (0,))).astype(BF16)
            total = base_ref[pair] + dot(half, s_ref[pair], ((1,), (0,)))
            inside = masks((rank_ref[pair] + 1) * RSTEP)
            lay_out(jnp.where(inside, total, 0.0), i, flat_ref, left_ref, right_ref)
        for j in range(CHUNKS):
            rows_ref[g, :, j * 128 : j * 128 + 128] = flat_ref[j * 8 : j * 8 + 8].astype(BF16)
        send(g).start()
        return _

    lax.fori_loop(0, groups, work, 0)
    for g in range(groups):
        send(g).wait()


def finish(ends, rank, at, s, own, base, groups):
    pairs = s.shape[0]
    return call(
        functools.partial(finish_kernel, count=len(groups)),
        [ANY] * 3 + [VMEM] * (3 + len(groups)),
        jax.ShapeDtypeStruct((pairs, R * R), BF16),
        HBM,
        [
            pltpu.VMEM((256, QP, 128), BF16),
            pltpu.VMEM((CHUNKS * 8, 128), F32),
            pltpu.VMEM((8, R, 128), F32),
            pltpu.VMEM((8, R, 128), F32),
            pltpu.VMEM((pairs // 8, 8, R * R), BF16),
            pltpu.SemaphoreType.DMA((pairs // 8,)),
            pltpu.SMEM(ends.shape, jnp.int32),
            pltpu.SMEM(rank.shape, jnp.int32),
            pltpu.SMEM(at.shape, jnp.int32),
            pltpu.SemaphoreType.DMA((3,)),
        ],
        pairs * 4 * R**3,
    )(ends, rank, at, s, own, base, *groups)


def added(*arrays):
    total = arrays[0].astype(F32)
    for a in arrays[1:]:
        total = total + a.astype(F32)
    return total.astype(BF16)


def sent_to_all(mine, tag):
    both = jnp.concatenate([mine, stage_z(mine, 1)], axis=0)
    group = [both] + [stage_b(both, d) for d in (1, 2, 3)]
    group = jnp.stack(group, axis=0)
    cuts = [(1, 0, 4), (2, 0, 4), (3, 0, 4)] if tag == "x" else [(1, 0, 4), (2, 0, 2), (2, 2, 4), (3, 0, 4)]
    groups = [group]
    for d, low, high in cuts:
        groups.append(stage_a(group[low:high], d))
    return groups + [stage_c(g) for g in groups]


def whole_step(pair_list, rank_bucket, amplitudes, intersects, integrals, exchange_blocks):
    at = jnp.stack([lax.axis_index(a) for a in AXES]).astype(jnp.int32)
    ends = pair_list.T

    block = pack(exchange_blocks)
    pair = jnp.stack([block, stage_z(block, EVEN[1])])
    far = stage_z(pair, EVEN[3])
    near = [pair[0], pair[1], far[1], far[0]]
    quarters = choose(at, near)
    blocks = sent_to_all(quarters, "x")

    m = relay(amplitudes)
    s = relay(intersects)
    p, *sums = project(ends, rank_bucket, at, s, m)
    v = relay(integrals)
    base = base_of(rank_bucket, m, v)

    sums = [added(sums[a], stage_c(sums[4 + a])) for a in (1, 3, 2, 0)]
    moved = [stage_a(sums[n], d) for n, d in enumerate((1, 3, 2))]
    sums = added(sums[3], *moved)
    sums = added(sums[0], *[stage_b(sums[d], d) for d in (1, 2, 3)])
    sums = added(sums[:4], stage_z(sums[4:], 1))
    parts = [sums] + [stage_z(sums, EVEN[d]) for d in (1, 2, 3)]
    near[0] = copied(near[0])
    coupled = couple(parts, near)
    own = own_of(ends, at, p, blocks)
    groups = sent_to_all(coupled, "g")
    return finish(ends, rank_bucket, at, s, own, base, groups)


def solution(mesh):
    torus = Mesh(mesh.devices.reshape(4, 2, mesh.shape["gy"], mesh.shape["gz"]), AXES)
    everywhere = P(AXES, None)
    return jax.shard_map(
        whole_step,
        mesh=torus,
        in_specs=(everywhere, P(AXES), everywhere, everywhere, everywhere, P(GX_GY, None)),
        out_specs=everywhere,
        check_vma=False,
    )
```
